32 devices in a mesh: region: 1, band: 32 (over z, y, x, core), tile: 1, sub: 1.
Axes of the slice: x: 2, y: 2, z: 4, core: 2. Of those that a mesh axis runs over, the one named last changes fastest.
Arguments:
- scenes: bfloat16 [60, 6, 1024, 128], P(('region', 'tile'), 'sub', 'band'), may hold values from -6 to 6
- clear_bits: int32 [2, 32, 256], P(('region', 'tile'), 'band'), may hold values from 0 to 1073741823
- footprint: int32 [60, 2], P(('region', 'tile')), may hold values from 0 to 31, as said below
- offsets: int32 [60, 2], P(('region', 'tile')), may hold values from 0 to 15
- acq_day: int32 [60], P(('region', 'tile')), may hold values from 0 to 364
Outputs:
- coefficients: float32 [8, 6, 128, 1024], P('region', 'sub', 'band', 'tile')
- monthly: float32 [12, 6, 128, 1024], P(('region', 'tile'), 'sub', 'band')
- annual: float32 [6, 128, 1024], P(('region', 'sub'), 'band', 'tile')
The draws below stay inside these ranges and needn't reach their ends.
Inputs may be any that keep to these rules, and one draw needn't show every extreme that they name: `clear_bits`: bit j (j < 30) of word w at cell (b, a) is 1 when date 30 w + j is clear over columns 4 b to 4 b + 3 and rows 4 a to 4 a + 3. footprint[t, 0] <= footprint[t, 1]; date t's scene covers columns 4 * footprint[t, 0] to 4 * (footprint[t, 1] + 1) - 1. `offsets`: offsets in sixteenths of a pixel, along rows then columns.
All inputs are finite; a program needn't handle non-finite values.
Results may differ from the reference program's by a relative error of at most 0.005.
Values may be sent and summed in bfloat16 or wider, within the bound.
No kernel may reach another device: no remote copies, remote signals or barrier semaphores. Data moves between devices by JAX's collectives and lax.ppermute only.
A program may use at most 64 MiB of HBM per device.

```python
import jax
import jax.numpy as jnp
from jax import lax

SPEC = 6
COLS_DEV = 4
DATES = 60
ROWS = 1024
COLS = 128
WORDS = 2


def draw_footprint(key, part):
    strip_count = COLS // COLS_DEV
    first_key, span_key = jax.random.split(jax.random.fold_in(key, 11))
    first_strip = jax.random.randint(first_key, (DATES,), 0, strip_count // 2 + 1)
    span_strip = jax.random.randint(span_key, (DATES,), strip_count // 4, strip_count)
    last_strip = jnp.minimum(first_strip + span_strip, strip_count - 1)
    return jnp.stack([first_strip, last_strip], axis=1).astype(jnp.int32)


def draw_acq_day(key, part):
    return jax.random.randint(jax.random.fold_in(key, 23), (DATES,), 0, 365).astype(jnp.int32)


def set_ends(result, own_key, low, high):
    longest = result.shape.index(max(result.shape))
    spots = []
    for shift in (0, 1):
        where = [jax.random.randint(jax.random.fold_in(own_key, axis), (), 0, length) for axis, length in enumerate(result.shape)]
        where[longest] = (where[longest] + shift) % result.shape[longest]
        spots.append(tuple(where))
    return result.at[spots[0]].set(low).at[spots[1]].set(high)


def levels(key, extent, cuts, least, high):
    loudness, own = 1.0, jax.random.fold_in(key, 6)
    for axis_at, blocks in cuts:
        steps = jnp.exp(jax.random.uniform(jax.random.fold_in(own, axis_at), (blocks,), jnp.float32, least / len(cuts), high / len(cuts)))
        loudness = loudness * jnp.repeat(steps, extent[axis_at] // blocks).reshape([-1 if axis == axis_at else 1 for axis in range(len(extent))])
    return loudness


def bell_draw(stream_key, extent, width, reach, cuts=(), kind=jnp.bfloat16):
    level = levels(stream_key, extent, cuts, -0.22, 0.18) if cuts else 1.0
    values = jax.random.normal(stream_key, extent, jnp.float32) * width * level
    return jnp.minimum(jnp.maximum(values, -reach), reach).astype(kind)


def setup_inputs(seed: int = 0, part: int = 0) -> dict:
    keys = jax.random.split(jax.random.key(seed), 6)
    part_splits = jax.random.split(jax.random.fold_in(keys[5], part), 6)
    return {
        "scenes": bell_draw(part_splits[0], (DATES, SPEC, ROWS, COLS), 1.0, 6.0, ((2, 32),)),
        "clear_bits": set_ends(jax.random.randint(part_splits[1], (WORDS, COLS // 4, ROWS // 4), 0, 1073741824), jax.random.fold_in(part_splits[1], 1), 0, 1073741823).astype(jnp.int32),
        "footprint": draw_footprint(jax.random.fold_in(jax.random.fold_in(keys[5], part), 71), part),
        "offsets": set_ends(jax.random.randint(part_splits[3], (DATES, 2), 0, 16), jax.random.fold_in(part_splits[3], 1), 0, 15).astype(jnp.int32),
        "acq_day": draw_acq_day(jax.random.fold_in(jax.random.fold_in(keys[5], part), 71), part),
    }


RIDGE = 1.0

def design_tables(acq_day):
    day_phase = acq_day.astype(jnp.float32) / 365.0
    columns = [jnp.ones_like(day_phase), 2.0 * day_phase - 1.0]
    for harmonic in (1, 2, 3):
        turn_angle = 2.0 * jnp.pi * harmonic * day_phase
        columns = columns + [jnp.cos(turn_angle), jnp.sin(turn_angle)]
    harmonic_basis = jnp.stack(columns, axis=1)
    month_index = acq_day * 12 // 365
    onehot = (month_index[:, None] == jnp.arange(12, dtype=jnp.int32)[None, :]).astype(jnp.float32)
    products = jnp.stack([harmonic_basis[:, row_term] * harmonic_basis[:, col_term] for row_term in range(8) for col_term in range(row_term + 1)], axis=1)
    return (jnp.concatenate([products, onehot], axis=1), jnp.concatenate([harmonic_basis, onehot], axis=1))

def bilinear(padded, offsets):
    shift_row = (offsets[:, 0].astype(jnp.float32) / 16.0)[:, None, None, None]
    shift_col = (offsets[:, 1].astype(jnp.float32) / 16.0)[:, None, None, None]
    upper_rows = padded[:, :, :-1].astype(jnp.float32)
    lower_rows = padded[:, :, 1:].astype(jnp.float32)

    def across(source):
        right_cell = jnp.concatenate([source[..., 1:], jnp.zeros_like(source[..., :1])], axis=-1)
        return (1.0 - shift_col) * source + shift_col * right_cell
    return ((1.0 - shift_row) * across(upper_rows) + shift_row * across(lower_rows)).astype(jnp.bfloat16)

def clear_weight(cell_words, footprint, col_start, strip_width):
    date_count = footprint.shape[0]
    per_date = jnp.repeat(cell_words, 30, axis=0)
    bit_place = (jnp.arange(date_count, dtype=jnp.int32) % 30)[:, None, None]
    clear_flag = jnp.right_shift(per_date, bit_place) & 1
    pixel_flag = jnp.repeat(jnp.repeat(clear_flag, 4, axis=1), 4, axis=2)
    strip_index = (col_start + jnp.arange(pixel_flag.shape[1], dtype=jnp.int32)) // strip_width
    covered = (strip_index[None, :] >= footprint[:, 0:1]) & (strip_index[None, :] <= footprint[:, 1:2])
    return pixel_flag.astype(jnp.float32) * covered[:, :, None].astype(jnp.float32)

def partial_sums(weight, values, common_table, banded_table):
    common = jnp.einsum('dxy,dk->kxy', weight, common_table, precision=lax.Precision.HIGHEST)
    weighted = values.astype(jnp.float32) * weight[:, None]
    banded = jnp.einsum('dsxy,dk->ksxy', weighted, banded_table, precision=lax.Precision.HIGHEST)
    return (common, banded)

def solve_normal(gram, rhs):
    pair_list = [(row_term, col_term) for row_term in range(8) for col_term in range(row_term + 1)]
    gram_entry = {}
    for position, term_pair in enumerate(pair_list):
        gram_entry[term_pair] = gram[position]
    factor = {}
    for col_term in range(8):
        pivot_value = gram_entry[col_term, col_term] + RIDGE
        for inner_term in range(col_term):
            pivot_value = pivot_value - factor[col_term, inner_term] * factor[col_term, inner_term]
        diag_root = jnp.sqrt(pivot_value)
        factor[col_term, col_term] = diag_root
        for row_term in range(col_term + 1, 8):
            running = gram_entry[row_term, col_term]
            for inner_term in range(col_term):
                running = running - factor[row_term, inner_term] * factor[col_term, inner_term]
            factor[row_term, col_term] = running / diag_root
    forward = []
    for row_term in range(8):
        running = rhs[row_term]
        for inner_term in range(row_term):
            running = running - factor[row_term, inner_term] * forward[inner_term]
        forward.append(running / factor[row_term, row_term])
    backward = [forward[0]] * 8
    for row_term in reversed(range(8)):
        running = forward[row_term]
        for inner_term in range(row_term + 1, 8):
            running = running - factor[inner_term, row_term] * backward[inner_term]
        backward[row_term] = running / factor[row_term, row_term]
    return jnp.stack(backward, axis=0)

def smooth_axis(padded_field, along):
    inner_size = padded_field.shape[along] - 2
    left_part = lax.slice_in_dim(padded_field, 0, inner_size, axis=along)
    centre_part = lax.slice_in_dim(padded_field, 1, inner_size + 1, axis=along)
    right_part = lax.slice_in_dim(padded_field, 2, inner_size + 2, axis=along)
    return 0.25 * left_part + 0.5 * centre_part + 0.25 * right_part

def reference(scenes, clear_bits, footprint, offsets, acq_day):
    padded = jnp.concatenate([scenes, jnp.zeros_like(scenes[:, :, 0:1, :])], axis=2)
    resampled = jnp.swapaxes(bilinear(padded, offsets), 2, 3)
    weight = clear_weight(clear_bits, footprint, 0, COLS_DEV)
    common_table, banded_table = design_tables(acq_day)
    common, banded = partial_sums(weight, resampled, common_table, banded_table)
    gram = common[:36]
    month_count = common[36:]
    rhs = banded[:8]
    month_sum = banded[8:]
    coefficients = solve_normal(gram, rhs)
    composite = month_sum / jnp.maximum(month_count, 1.0)[:, None]
    yearly = lax.optimization_barrier(jnp.sum(month_sum, axis=0)) / jnp.maximum(lax.optimization_barrier(jnp.sum(month_count, axis=0)), 1.0)
    month_pad = jnp.pad(composite, ((0, 0), (0, 0), (1, 1), (1, 1)))
    monthly = smooth_axis(smooth_axis(month_pad, 3), 2)
    year_pad = jnp.pad(yearly, ((0, 0), (1, 1), (1, 1)))
    annual = smooth_axis(smooth_axis(year_pad, 2), 1)
    return (coefficients, monthly, annual)
```

```python
import functools

import jax
import jax.numpy as jnp
import numpy as np
from jax import lax
from jax.experimental import pallas as pl
from jax.experimental.pallas import tpu as pltpu
from jax.sharding import PartitionSpec as P

RIDGE = 1.0


def shifted(value, axis, steps):
    count = lax.axis_size(axis)
    first, last = (max(0, -steps), min(count, count - steps))
    return lax.ppermute(value, axis, [(source, source + steps) for source in range(first, last)])


def extended(x, sides, width):
    for axis, dim in sides:
        devices, length = (lax.axis_size(axis), x.shape[dim])
        up = [(i, (i + 1) % devices) for i in range(devices - 1)]
        down = [(j, i) for i, j in up]
        last = lax.slice_in_dim(x, length - width, length, axis=dim)
        first = lax.slice_in_dim(x, 0, width, axis=dim)
        before = lax.ppermute(last, axis, up)
        after = lax.ppermute(first, axis, down)
        x = jnp.concatenate([before, x, after], axis=dim)
    return x


def design_tables(acq_day):
    day_phase = acq_day.astype(jnp.float32) / 365.0
    columns = [jnp.ones_like(day_phase), 2.0 * day_phase - 1.0]
    for harmonic in (1, 2, 3):
        turn_angle = 2.0 * jnp.pi * harmonic * day_phase
        columns = columns + [jnp.cos(turn_angle), jnp.sin(turn_angle)]
    harmonic_basis = jnp.stack(columns, axis=1)
    month_index = acq_day * 12 // 365
    onehot = (month_index[:, None] == jnp.arange(12, dtype=jnp.int32)[None, :]).astype(jnp.float32)
    products = jnp.stack(
        [
            harmonic_basis[:, row_term] * harmonic_basis[:, col_term]
            for row_term in range(8)
            for col_term in range(row_term + 1)
        ],
        axis=1,
    )
    return (
        jnp.concatenate([products, onehot], axis=1),
        jnp.concatenate([harmonic_basis, onehot], axis=1),
    )


def bilinear(padded, offsets):
    shift_row = (offsets[:, 0].astype(jnp.float32) / 16.0)[:, None, None, None]
    shift_col = (offsets[:, 1].astype(jnp.float32) / 16.0)[:, None, None, None]
    upper_rows = padded[:, :, :-1].astype(jnp.float32)
    lower_rows = padded[:, :, 1:].astype(jnp.float32)

    def across(source):
        right_cell = jnp.concatenate([source[..., 1:], jnp.zeros_like(source[..., :1])], axis=-1)
        return (1.0 - shift_col) * source + shift_col * right_cell

    return ((1.0 - shift_row) * across(upper_rows) + shift_row * across(lower_rows)).astype(
        jnp.bfloat16
    )


def clear_weight(cell_words, footprint, strip_width):
    date_count = footprint.shape[0]
    per_date = jnp.repeat(cell_words, 30, axis=0)
    bit_place = (jnp.arange(date_count, dtype=jnp.int32) % 30)[:, None, None]
    clear_flag = jnp.right_shift(per_date, bit_place) & 1
    pixel_flag = jnp.repeat(jnp.repeat(clear_flag, 4, axis=1), 4, axis=2)
    strip_index = jnp.arange(pixel_flag.shape[1], dtype=jnp.int32) // strip_width
    covered = (strip_index[None, :] >= footprint[:, 0:1]) & (
        strip_index[None, :] <= footprint[:, 1:2]
    )
    return pixel_flag.astype(jnp.float32) * covered[:, :, None].astype(jnp.float32)


def partial_sums(weight, values, common_table, banded_table):
    common = jnp.einsum("dxy,dk->kxy", weight, common_table, precision=lax.Precision.HIGHEST)
    weighted = values.astype(jnp.float32) * weight[:, None]
    banded = jnp.einsum("dsxy,dk->ksxy", weighted, banded_table, precision=lax.Precision.HIGHEST)
    return (common, banded)


def solve_normal(gram, rhs):
    pair_list = [(row_term, col_term) for row_term in range(8) for col_term in range(row_term + 1)]
    gram_entry = {}
    for position, term_pair in enumerate(pair_list):
        gram_entry[term_pair] = gram[position]
    factor = {}
    for col_term in range(8):
        pivot_value = gram_entry[col_term, col_term] + RIDGE
        for inner_term in range(col_term):
            pivot_value = pivot_value - factor[col_term, inner_term] * factor[col_term, inner_term]
        diag_root = jnp.sqrt(pivot_value)
        factor[col_term, col_term] = diag_root
        for row_term in range(col_term + 1, 8):
            running = gram_entry[row_term, col_term]
            for inner_term in range(col_term):
                running = running - factor[row_term, inner_term] * factor[col_term, inner_term]
            factor[row_term, col_term] = running / diag_root
    forward = []
    for row_term in range(8):
        running = rhs[row_term]
        for inner_term in range(row_term):
            running = running - factor[row_term, inner_term] * forward[inner_term]
        forward.append(running / factor[row_term, row_term])
    backward = [forward[0]] * 8
    for row_term in reversed(range(8)):
        running = forward[row_term]
        for inner_term in range(row_term + 1, 8):
            running = running - factor[inner_term, row_term] * backward[inner_term]
        backward[row_term] = running / factor[row_term, row_term]
    return jnp.stack(backward, axis=0)


def smooth_axis(padded_field, along):
    inner_size = padded_field.shape[along] - 2
    left_part = lax.slice_in_dim(padded_field, 0, inner_size, axis=along)
    centre_part = lax.slice_in_dim(padded_field, 1, inner_size + 1, axis=along)
    right_part = lax.slice_in_dim(padded_field, 2, inner_size + 2, axis=along)
    return 0.25 * left_part + 0.5 * centre_part + 0.25 * right_part


def split_dates(scenes, clear_bits, footprint, offsets, acq_day):
    date_count, band_count, row_local, col_count = scenes.shape
    strip_count = lax.axis_size("band")
    tile_count = lax.axis_size("tile")
    strip_width = col_count // strip_count
    row_count = row_local * strip_count
    common_table, banded_table = design_tables(acq_day)
    below = shifted(scenes[:, :, 0:1, :], "band", -1)
    resampled = bilinear(jnp.concatenate([scenes, below], axis=2), offsets)
    flipped = jnp.swapaxes(resampled, 2, 3)
    cell_words = lax.all_to_all(clear_bits, "band", split_axis=2, concat_axis=1, tiled=True)
    weight = clear_weight(cell_words, footprint, strip_width)
    common, banded = partial_sums(weight, flipped, common_table, banded_table)
    common, banded = (
        lax.all_to_all(common, "band", split_axis=1, concat_axis=2, tiled=True),
        lax.all_to_all(
            banded.reshape(-1, col_count, row_local),
            "band",
            split_axis=1,
            concat_axis=2,
            tiled=True,
        ),
    )
    banded = banded.reshape(20, band_count, strip_width, row_count)
    gram = common[:36]
    month_count = common[36:]
    rhs = banded[:8]
    month_sum = banded[8:]
    annual_sum = jnp.sum(month_sum, axis=0)
    annual_count = jnp.sum(month_count, axis=0)
    month_sum, month_count = (
        lax.psum_scatter(month_sum, "tile", scatter_dimension=0, tiled=True),
        lax.psum_scatter(month_count, "tile", scatter_dimension=0, tiled=True),
    )
    composite = month_sum / jnp.maximum(month_count, 1.0)[:, None]
    month_edged = extended(composite, (("band", 2),), 1)
    month_edged = jnp.pad(month_edged, ((0, 0), (0, 0), (0, 0), (1, 1)))
    monthly = smooth_axis(smooth_axis(month_edged, 3), 2)
    share = row_count // tile_count
    gram, rhs, annual_sum, annual_count = lax.psum((gram, rhs, annual_sum, annual_count), "tile")
    start = lax.axis_index("tile") * share
    gram = lax.dynamic_slice_in_dim(gram, start, share, 2)
    rhs = lax.dynamic_slice_in_dim(rhs, start, share, 3)
    annual_sum = lax.dynamic_slice_in_dim(annual_sum, start, share, 2)
    annual_count = lax.dynamic_slice_in_dim(annual_count, start, share, 1)
    coefficients = solve_normal(gram, rhs)
    yearly = annual_sum / jnp.maximum(annual_count, 1.0)
    year_edged = extended(yearly, (("band", 1), ("tile", 2)), 1)
    annual = smooth_axis(smooth_axis(year_edged, 2), 1)
    return (coefficients, monthly, annual)


def cdiv(a, b):
    return -(-a // b)


def lane_iota(shape, dim):
    return lax.broadcasted_iota(jnp.int32, shape, dim)


def resample_body(group, offs_ref, day_ref, scenes_ref, below_ref, x_ref, bk_ref, pk_ref):
    dates, bands, rows, cols = scenes_ref.shape
    step = pl.program_id(0)
    not_last = lane_iota((1, cols), 1) < cols - 1
    bottom = lane_iota((rows, cols), 0) == rows - 1

    def splat(value):
        return jnp.full((1, cols), value, jnp.int32).astype(jnp.float32) * (1.0 / 16.0)

    def pair(tp, carry):
        fractions = []
        for u in (0, 1):
            t = 2 * tp + u
            fy, fx = (splat(offs_ref[step * dates + t, i]) for i in (0, 1))
            keep, take = 1.0 - fx, jnp.where(not_last, fx, 0.0)
            edge = below_ref[t].astype(jnp.float32)
            edge = keep * edge + take * pltpu.roll(edge, cols - 1, 1)
            fractions.append((fy, keep, take, edge))
        for s in range(bands):
            halves = []
            for u in (0, 1):
                fy, keep, take, edge = fractions[u]
                source = scenes_ref[2 * tp + u, s].astype(jnp.float32)
                across = keep * source + take * pltpu.roll(source, cols - 1, 1)
                lower = jnp.where(bottom, edge[s : s + 1], pltpu.roll(across, rows - 1, 0))
                halves.append((1.0 - fy) * across + fy * lower)
            for part in range(rows // 8):
                q, g = divmod(part, group)
                tile = jnp.concatenate([half[8 * part : 8 * part + 8] for half in halves], axis=0)
                x_ref[q, s, pl.ds(pl.multiple_of(16 * tp, 16), 16), g * cols : (g + 1) * cols] = tile.astype(
                    jnp.bfloat16
                )
        return carry

    lax.fori_loop(0, dates // 2, pair, 0)

    @pl.when(step == 0)
    def _():
        width = bk_ref.shape[1]
        owner = lane_iota((1, width), 1) // 8
        day = lax.fori_loop(
            0, width // 8, lambda t, d: jnp.where(owner == t, day_ref[t], d), jnp.zeros((1, width), jnp.int32)
        )
        phase = day.astype(jnp.float32) / 365.0
        basis = [jnp.ones_like(phase), 2.0 * phase - 1.0]
        for harmonic in (1, 2, 3):
            angle = 2.0 * jnp.pi * harmonic * phase
            basis = basis + [jnp.cos(angle), jnp.sin(angle)]
        months = [
            jnp.where((12 * day >= 365 * m) & (12 * day < 365 * (m + 1)), 1.0, 0.0) for m in range(12)
        ]

        def coarse(row):
            return row.astype(jnp.bfloat16).astype(jnp.float32)

        def split(entries):
            high = [coarse(row) for row in entries]
            return high + [row - top for row, top in zip(entries, high)]

        products = [basis[i] * basis[j] for i in range(8) for j in range(i + 1)]
        diagonal = lane_iota((8, width), 1) % 8 == lane_iota((8, width), 0)
        for ref, entries in ((bk_ref, split(basis[1:]) + months), (pk_ref, split(products) + months)):
            for k in range(0, len(entries), 2):
                tile = jnp.concatenate(
                    [jnp.where(diagonal, jnp.broadcast_to(row, (8, width)), 0.0) for row in entries[k : k + 2]],
                    axis=0,
                )
                ref[8 * k : 8 * k + 16] = tile.astype(jnp.bfloat16)


def fit_body(
    cell, words, place_ref, foot_ref, bits_ref, x_ref, bk_ref, pk_ref, smooth_ref, send_ref, b8, w_ref, g_ref, inv_ref, y_ref
):
    _, bands, depth, wide = x_ref.shape
    strips, _, lanes = bits_ref.shape
    cols = send_ref.shape[2]
    group = wide // cols
    cells_here = b8.shape[1]
    strip_width = cols // strips
    q = pl.program_id(0)
    per_word = depth // 8 // words
    f32 = jnp.float32

    @pl.when(q == 0)
    def _():
        band = place_ref[0]
        first = band * cells_here
        block, within = first // lanes, lax.rem(first, lanes)
        blocks = bits_ref.shape[1] // words
        mine = jnp.where(
            lane_iota((strips, cols), 1) // strip_width == lane_iota((strips, cols), 0), 1.0, 0.0
        ).astype(jnp.bfloat16)
        for w in range(words):
            word = bits_ref[:, blocks * w, :]
            for other in range(1, blocks):
                word = jnp.where(block == other, bits_ref[:, blocks * w + other, :], word)
            word = pltpu.roll(word, lanes - within, 1)
            total = jnp.zeros((cells_here, cols), jnp.int32)
            for shift in (0, 8, 16, 24):
                piece = (lax.shift_right_logical(word, shift) & 255).astype(f32).astype(jnp.bfloat16)
                spread = lax.dot_general(piece, mine, (((0,), (0,)), ((), ())), preferred_element_type=f32)
                total = total + (spread[:cells_here].astype(jnp.int32) << shift)
            b8[w] = total
        y_ref[...] = jnp.zeros_like(y_ref)

    strip = lane_iota((8, wide), 1) % cols // strip_width
    upper = lane_iota((8, cols), 0) < cell
    for w in range(words):
        pieces = []
        for g in range(group):
            base = (q * group + g) * (8 // cell)
            pieces.append(
                jnp.where(upper, b8[w, pl.ds(base, 1), :], b8[w, pl.ds(base + 1, 1), :])
            )
        word = jnp.concatenate(pieces, axis=1)

        def mask_pair(tp, carry, w=w, word=word):
            tiles = []
            for u in (0, 1):
                bit = 2 * tp + u
                t = w * per_word + bit
                covered = (strip >= foot_ref[t, 0]) & (strip <= foot_ref[t, 1])
                flag = lax.shift_right_logical(word, jnp.full((8, wide), bit, jnp.int32)) & 1
                tiles.append(jnp.where(covered, flag, 0).astype(f32))
            row = pl.multiple_of(w * per_word * 8 + 16 * tp, 16)
            w_ref[pl.ds(row, 16), :] = jnp.concatenate(tiles, axis=0).astype(jnp.bfloat16)
            return carry

        lax.fori_loop(0, per_word // 2, mask_pair, 0)

    weight = w_ref[...]
    g_ref[...] = jnp.dot(pk_ref[...], weight, preferred_element_type=f32)
    pairs = [(i, j) for i in range(8) for j in range(i + 1)]
    gram = {
        ij: g_ref[8 * n : 8 * n + 8] + g_ref[8 * (n + 36) : 8 * (n + 36) + 8] for n, ij in enumerate(pairs)
    }
    factor, inverse_root = {}, {}
    for j in range(8):
        pivot = gram[j, j] + RIDGE
        for k in range(j):
            pivot = pivot - factor[j, k] * factor[j, k]
        inverse_root[j] = lax.rsqrt(pivot)
        for i in range(j + 1, 8):
            running = gram[i, j]
            for k in range(j):
                running = running - factor[i, k] * factor[j, k]
            factor[i, j] = running * inverse_root[j]
    lower = {}
    for j in range(8):
        lower[j, j] = inverse_root[j]
        for i in range(j + 1, 8):
            running = factor[i, j] * lower[j, j]
            for k in range(j + 1, i):
                running = running + factor[i, k] * lower[k, j]
            lower[i, j] = -running * inverse_root[i]
    for n, (i, j) in enumerate(pairs):
        total = lower[i, i] * lower[i, j]
        for k in range(i + 1, 8):
            total = total + lower[k, i] * lower[k, j]
        inv_ref[8 * n : 8 * n + 8] = total
    index = {ij: n for n, ij in enumerate(pairs)}

    def inverse(i, j):
        n = index[max(i, j), min(i, j)]
        return inv_ref[8 * n : 8 * n + 8]

    counts = [g_ref[8 * (72 + m) : 8 * (72 + m) + 8] for m in range(12)]
    total_count = counts[0]
    for m in range(1, 12):
        total_count = total_count + counts[m]
    for m in range(12):
        g_ref[8 * m : 8 * m + 8] = 1.0 / jnp.maximum(counts[m], 1.0)
    g_ref[96:104] = 1.0 / jnp.maximum(total_count, 1.0)

    coef_groups = cdiv(8 * bands, 16)

    def put(base, v, value):
        at, rest = divmod(v, 16)
        h, rest = divmod(rest, 8)
        e, p = divmod(rest, 4)
        rows = group * 8
        span = y_ref.shape[1] // 8
        tall = jnp.concatenate([value[:, g * cols : (g + 1) * cols] for g in range(group)], axis=0)
        row = pl.multiple_of((4 * h + p) * span + q * rows, rows)
        y_ref[base + at, pl.ds(row, rows), e * cols : (e + 1) * cols] = tall.astype(jnp.bfloat16)

    for s in range(bands):
        sums = jnp.dot(bk_ref[...], x_ref[0, s] * weight, preferred_element_type=f32)
        month = [sums[8 * (14 + m) : 8 * (14 + m) + 8] for m in range(12)]
        whole = month[0]
        for m in range(1, 12):
            whole = whole + month[m]
        rhs = [whole] + [sums[8 * k : 8 * k + 8] + sums[8 * (k + 7) : 8 * (k + 7) + 8] for k in range(7)]
        for i in range(8):
            value = inverse(i, 0) * rhs[0]
            for j in range(1, 8):
                value = value + inverse(i, j) * rhs[j]
            put(0, i * bands + s, value)
        for m in range(12):
            put(coef_groups, m * bands + s, month[m] * g_ref[8 * m : 8 * m + 8])
        put(coef_groups, 12 * bands + s, whole * g_ref[96:104])

    @pl.when(q == pl.num_programs(0) - 1)
    def _():
        for at in range(y_ref.shape[0]):
            turned = lax.dot_general(
                smooth_ref[0 if at < coef_groups else 1],
                y_ref[at],
                (((1,), (1,)), ((), ())),
                preferred_element_type=f32,
            ).reshape(strips, 2 * strip_width, 2 * cols)
            tile = jnp.concatenate([turned[:, :, :cols], turned[:, :, cols:]], axis=1)
            send_ref[:, 16 * at : 16 * at + 16, :] = tile.astype(jnp.bfloat16)


def finish_body(bands, recv_ref, coef_ref, month_ref, year_ref):
    strips, _, lanes = recv_ref.shape
    coef_groups = cdiv(8 * bands, 16)
    month_groups = cdiv(13 * bands, 16)
    quarter = lanes // 4
    lane = lane_iota((16, lanes), 1)
    low_half = lane < 2 * quarter
    even = lane // quarter % 2 == 0
    for at in range(coef_groups + month_groups):
        tiles = []
        for lt in range(strips // 4):
            x = [recv_ref[4 * lt + b, 16 * at : 16 * at + 16, :].astype(jnp.float32) for b in range(4)]
            for b in (0, 1):
                first, second = x[b], x[b + 2]
                x[b] = jnp.where(low_half, first, pltpu.roll(second, 2 * quarter, 1))
                x[b + 2] = jnp.where(low_half, pltpu.roll(first, 2 * quarter, 1), second)
            for b in (0, 2):
                first, second = x[b], x[b + 1]
                x[b] = jnp.where(even, first, pltpu.roll(second, quarter, 1))
                x[b + 1] = jnp.where(even, pltpu.roll(first, 3 * quarter, 1), second)
            tiles.append(x)
        for p in range(4):
            field = jnp.concatenate([tile[p] for tile in tiles], axis=1)
            if at >= coef_groups:
                full = field.shape[1]
                where = lane_iota(field.shape, 1)
                before = jnp.where(where == 0, 0.0, pltpu.roll(field, 1, 1))
                after = jnp.where(where == full - 1, 0.0, pltpu.roll(field, full - 1, 1))
                field = 0.25 * before + 0.5 * field + 0.25 * after
            for e in range(4):
                v = 16 * (at if at < coef_groups else at - coef_groups) + 4 * e + p
                piece = field[4 * e : 4 * e + 4]
                if at < coef_groups:
                    if v < 8 * bands:
                        coef_ref[v] = piece
                elif v < 12 * bands:
                    month_ref[v] = piece
                elif v < 13 * bands:
                    year_ref[v - 12 * bands] = piece


def turn_tables(strips, strip_width):
    cols = strips * strip_width
    row, col = np.arange(2 * cols)[:, None], np.arange(2 * cols)[None, :]
    column = strip_width * (row // (2 * strip_width)) + row % strip_width
    same = row // strip_width % 2 == col // cols
    apart = np.abs(column - col % cols)
    plain = np.where(same & (apart == 0), 1.0, 0.0)
    smooth = np.where(same, np.where(apart == 0, 0.5, np.where(apart == 1, 0.25, 0.0)), 0.0)
    return jnp.asarray(np.stack([plain, smooth]), jnp.bfloat16)


def whole_dates(scenes, clear_bits, footprint, offsets, acq_day):
    dates, bands, rows, cols = scenes.shape
    words, _, cells = clear_bits.shape
    strips = lax.axis_size("band")
    strip_width = cols // strips
    cell = rows * strips // cells
    group, lanes = 2, 128
    steps = rows // 8 // group
    chunk = 12
    depth = 8 * dates
    f32, bf16 = jnp.float32, jnp.bfloat16
    below = shifted(scenes[:, :, 0, :], "band", -1)
    flags = jnp.broadcast_to(clear_bits.reshape(1, words * cells // lanes, lanes), (strips, words * cells // lanes, lanes))
    flags = lax.all_to_all(flags, "band", split_axis=0, concat_axis=0, tiled=True)
    smem = pl.BlockSpec(memory_space=pltpu.SMEM)

    def held(shape):
        return pl.BlockSpec(shape, lambda i: (0,) * len(shape))

    table_rows, product_rows = 8 * 26, 8 * 84
    resampled, table, product = pl.pallas_call(
        functools.partial(resample_body, group),
        grid=(dates // chunk,),
        in_specs=[
            smem,
            smem,
            pl.BlockSpec((chunk, bands, rows, cols), lambda i: (i, 0, 0, 0)),
            pl.BlockSpec((chunk, bands, cols), lambda i: (i, 0, 0)),
        ],
        out_specs=[
            pl.BlockSpec((steps, bands, 8 * chunk, group * cols), lambda i: (0, 0, i, 0)),
            held((table_rows, depth)),
            held((product_rows, depth)),
        ],
        out_shape=[
            jax.ShapeDtypeStruct((steps, bands, depth, group * cols), bf16),
            jax.ShapeDtypeStruct((table_rows, depth), bf16),
            jax.ShapeDtypeStruct((product_rows, depth), bf16),
        ],
        cost_estimate=pl.CostEstimate(flops=20_000_000, bytes_accessed=6_000_000, transcendentals=0),
        name="resample",
    )(offsets, acq_day, scenes, below)
    groups = cdiv(8 * bands, 16) + cdiv(13 * bands, 16)
    place = lax.axis_index("band").reshape(1).astype(jnp.int32)
    send = pl.pallas_call(
        functools.partial(fit_body, cell, words),
        grid=(steps,),
        in_specs=[
            smem,
            smem,
            held(flags.shape),
            pl.BlockSpec((1, bands, depth, group * cols), lambda i: (i, 0, 0, 0)),
            held((table_rows, depth)),
            held((product_rows, depth)),
            held((2, 2 * cols, 2 * cols)),
        ],
        out_specs=held((strips, 16 * groups, 4 * rows)),
        out_shape=jax.ShapeDtypeStruct((strips, 16 * groups, 4 * rows), bf16),
        scratch_shapes=[
            pltpu.VMEM((words, rows // cell, cols), jnp.int32),
            pltpu.VMEM((depth, group * cols), bf16),
            pltpu.VMEM((product_rows, group * cols), f32),
            pltpu.VMEM((8 * 36, group * cols), f32),
            pltpu.VMEM((groups, 8 * rows, 2 * cols), bf16),
        ],
        cost_estimate=pl.CostEstimate(flops=20_000_000, bytes_accessed=6_000_000, transcendentals=0),
        name="fit",
    )(place, footprint, flags, resampled, table, product, turn_tables(strips, strip_width))
    received = lax.all_to_all(send, "band", split_axis=0, concat_axis=0, tiled=True)
    row_count = rows * strips
    shapes = [(n * bands, strip_width, row_count) for n in (8, 12, 1)]
    coefficients, monthly, annual = pl.pallas_call(
        functools.partial(finish_body, bands),
        out_shape=[jax.ShapeDtypeStruct(shape, f32) for shape in shapes],
        name="finish",
    )(received)
    return (
        coefficients.reshape(8, bands, strip_width, row_count),
        monthly.reshape(12, bands, strip_width, row_count),
        annual,
    )


def shards(scenes, clear_bits, footprint, offsets, acq_day):
    dates, _, rows, cols = scenes.shape
    strips = lax.axis_size("band")
    cells = clear_bits.shape[2]
    whole = (
        lax.axis_size("tile") == 1
        and cols == 128
        and rows == 32
        and cols == 4 * strips
        and cells == 8 * strips
        and dates % 12 == 0
    )
    plan = whole_dates if whole else split_dates
    return plan(scenes, clear_bits, footprint, offsets, acq_day)


def solution(mesh):
    placed = (
        P(("region", "tile"), "sub", "band", None),
        P(("region", "tile"), "band", None),
        P(("region", "tile"), None),
        P(("region", "tile"), None),
        P(("region", "tile")),
    )
    return jax.shard_map(
        shards,
        mesh=mesh,
        in_specs=placed,
        out_specs=(
            P("region", "sub", "band", "tile"),
            P(("region", "tile"), "sub", "band", None),
            P(("region", "sub"), "band", "tile"),
        ),
        check_vma=False,
    )
```

```python
import functools

import jax
import jax.numpy as jnp
import numpy as np
from jax import lax
from jax.experimental import pallas as pl
from jax.experimental.pallas import tpu as pltpu
from jax.sharding import PartitionSpec as P

RIDGE = 1.0
STRIP = 4
TABLE = 8 * 26
PRODUCT = 8 * 84
EDGES = 64
FIT_VMEM = 60 * 1024 * 1024 - (8 << 20)


def shifted(value, axis, steps):
    count = lax.axis_size(axis)
    first, last = (max(0, -steps), min(count, count - steps))
    return lax.ppermute(value, axis, [(source, source + steps) for source in range(first, last)])


def extended(x, sides, width):
    for axis, dim in sides:
        devices, length = (lax.axis_size(axis), x.shape[dim])
        up = [(i, (i + 1) % devices) for i in range(devices - 1)]
        down = [(j, i) for i, j in up]
        last = lax.slice_in_dim(x, length - width, length, axis=dim)
        first = lax.slice_in_dim(x, 0, width, axis=dim)
        before = lax.ppermute(last, axis, up)
        after = lax.ppermute(first, axis, down)
        x = jnp.concatenate([before, x, after], axis=dim)
    return x


def design_tables(acq_day):
    day_phase = acq_day.astype(jnp.float32) / 365.0
    columns = [jnp.ones_like(day_phase), 2.0 * day_phase - 1.0]
    for harmonic in (1, 2, 3):
        turn_angle = 2.0 * jnp.pi * harmonic * day_phase
        columns = columns + [jnp.cos(turn_angle), jnp.sin(turn_angle)]
    harmonic_basis = jnp.stack(columns, axis=1)
    month_index = acq_day * 12 // 365
    onehot = (month_index[:, None] == jnp.arange(12, dtype=jnp.int32)[None, :]).astype(jnp.float32)
    products = jnp.stack(
        [
            harmonic_basis[:, row_term] * harmonic_basis[:, col_term]
            for row_term in range(8)
            for col_term in range(row_term + 1)
        ],
        axis=1,
    )
    return (
        jnp.concatenate([products, onehot], axis=1),
        jnp.concatenate([harmonic_basis, onehot], axis=1),
    )


def bilinear(padded, offsets):
    shift_row = (offsets[:, 0].astype(jnp.float32) / 16.0)[:, None, None, None]
    shift_col = (offsets[:, 1].astype(jnp.float32) / 16.0)[:, None, None, None]
    upper_rows = padded[:, :, :-1].astype(jnp.float32)
    lower_rows = padded[:, :, 1:].astype(jnp.float32)

    def across(source):
        right_cell = jnp.concatenate([source[..., 1:], jnp.zeros_like(source[..., :1])], axis=-1)
        return (1.0 - shift_col) * source + shift_col * right_cell

    return ((1.0 - shift_row) * across(upper_rows) + shift_row * across(lower_rows)).astype(
        jnp.bfloat16
    )


def clear_weight(cell_words, footprint, strip_width):
    date_count = footprint.shape[0]
    per_date = jnp.repeat(cell_words, 30, axis=0)
    bit_place = (jnp.arange(date_count, dtype=jnp.int32) % 30)[:, None, None]
    clear_flag = jnp.right_shift(per_date, bit_place) & 1
    pixel_flag = jnp.repeat(jnp.repeat(clear_flag, 4, axis=1), 4, axis=2)
    strip_index = jnp.arange(pixel_flag.shape[1], dtype=jnp.int32) // strip_width
    covered = (strip_index[None, :] >= footprint[:, 0:1]) & (
        strip_index[None, :] <= footprint[:, 1:2]
    )
    return pixel_flag.astype(jnp.float32) * covered[:, :, None].astype(jnp.float32)


def partial_sums(weight, values, common_table, banded_table):
    common = jnp.einsum("dxy,dk->kxy", weight, common_table, precision=lax.Precision.HIGHEST)
    weighted = values.astype(jnp.float32) * weight[:, None]
    banded = jnp.einsum("dsxy,dk->ksxy", weighted, banded_table, precision=lax.Precision.HIGHEST)
    return (common, banded)


def solve_normal(gram, rhs):
    pair_list = [(row_term, col_term) for row_term in range(8) for col_term in range(row_term + 1)]
    gram_entry = {}
    for position, term_pair in enumerate(pair_list):
        gram_entry[term_pair] = gram[position]
    factor = {}
    for col_term in range(8):
        pivot_value = gram_entry[col_term, col_term] + RIDGE
        for inner_term in range(col_term):
            pivot_value = pivot_value - factor[col_term, inner_term] * factor[col_term, inner_term]
        diag_root = jnp.sqrt(pivot_value)
        factor[col_term, col_term] = diag_root
        for row_term in range(col_term + 1, 8):
            running = gram_entry[row_term, col_term]
            for inner_term in range(col_term):
                running = running - factor[row_term, inner_term] * factor[col_term, inner_term]
            factor[row_term, col_term] = running / diag_root
    forward = []
    for row_term in range(8):
        running = rhs[row_term]
        for inner_term in range(row_term):
            running = running - factor[row_term, inner_term] * forward[inner_term]
        forward.append(running / factor[row_term, row_term])
    backward = [forward[0]] * 8
    for row_term in reversed(range(8)):
        running = forward[row_term]
        for inner_term in range(row_term + 1, 8):
            running = running - factor[inner_term, row_term] * backward[inner_term]
        backward[row_term] = running / factor[row_term, row_term]
    return jnp.stack(backward, axis=0)


def smooth_axis(padded_field, along):
    inner_size = padded_field.shape[along] - 2
    left_part = lax.slice_in_dim(padded_field, 0, inner_size, axis=along)
    centre_part = lax.slice_in_dim(padded_field, 1, inner_size + 1, axis=along)
    right_part = lax.slice_in_dim(padded_field, 2, inner_size + 2, axis=along)
    return 0.25 * left_part + 0.5 * centre_part + 0.25 * right_part


def split_dates(scenes, clear_bits, footprint, offsets, acq_day):
    date_count, band_count, row_local, col_count = scenes.shape
    strip_count = lax.axis_size("band")
    tile_count = lax.axis_size("tile")
    strip_width = col_count // strip_count
    row_count = row_local * strip_count
    common_table, banded_table = design_tables(acq_day)
    below = shifted(scenes[:, :, 0:1, :], "band", -1)
    resampled = bilinear(jnp.concatenate([scenes, below], axis=2), offsets)
    flipped = jnp.swapaxes(resampled, 2, 3)
    cell_words = lax.all_to_all(clear_bits, "band", split_axis=2, concat_axis=1, tiled=True)
    weight = clear_weight(cell_words, footprint, strip_width)
    common, banded = partial_sums(weight, flipped, common_table, banded_table)
    common, banded = (
        lax.all_to_all(common, "band", split_axis=1, concat_axis=2, tiled=True),
        lax.all_to_all(
            banded.reshape(-1, col_count, row_local),
            "band",
            split_axis=1,
            concat_axis=2,
            tiled=True,
        ),
    )
    banded = banded.reshape(20, band_count, strip_width, row_count)
    gram = common[:36]
    month_count = common[36:]
    rhs = banded[:8]
    month_sum = banded[8:]
    annual_sum = jnp.sum(month_sum, axis=0)
    annual_count = jnp.sum(month_count, axis=0)
    month_sum, month_count = (
        lax.psum_scatter(month_sum, "tile", scatter_dimension=0, tiled=True),
        lax.psum_scatter(month_count, "tile", scatter_dimension=0, tiled=True),
    )
    composite = month_sum / jnp.maximum(month_count, 1.0)[:, None]
    month_edged = extended(composite, (("band", 2),), 1)
    month_edged = jnp.pad(month_edged, ((0, 0), (0, 0), (0, 0), (1, 1)))
    monthly = smooth_axis(smooth_axis(month_edged, 3), 2)
    share = row_count // tile_count
    gram, rhs, annual_sum, annual_count = lax.psum((gram, rhs, annual_sum, annual_count), "tile")
    start = lax.axis_index("tile") * share
    gram = lax.dynamic_slice_in_dim(gram, start, share, 2)
    rhs = lax.dynamic_slice_in_dim(rhs, start, share, 3)
    annual_sum = lax.dynamic_slice_in_dim(annual_sum, start, share, 2)
    annual_count = lax.dynamic_slice_in_dim(annual_count, start, share, 1)
    coefficients = solve_normal(gram, rhs)
    yearly = annual_sum / jnp.maximum(annual_count, 1.0)
    year_edged = extended(yearly, (("band", 1), ("tile", 2)), 1)
    annual = smooth_axis(smooth_axis(year_edged, 2), 1)
    return (coefficients, monthly, annual)


def cdiv(a, b):
    return -(-a // b)


def lane_iota(shape, dim):
    return lax.broadcasted_iota(jnp.int32, shape, dim)


def fit_rows(day):
    phase = day / 365.0
    turn = 2.0 * jnp.pi * phase
    c, s = jnp.cos(turn), jnp.sin(turn)
    basis = [
        jnp.ones_like(phase),
        2.0 * phase - 1.0,
        c,
        s,
        2.0 * c * c - 1.0,
        2.0 * s * c,
        (4.0 * c * c - 3.0) * c,
        (3.0 - 4.0 * s * s) * s,
    ]
    months = [
        jnp.where((12.0 * day >= 365.0 * m) & (12.0 * day < 365.0 * (m + 1)), 1.0, 0.0) for m in range(12)
    ]
    return basis, months


def two_parts(entries):
    high = [row.astype(jnp.bfloat16).astype(jnp.float32) for row in entries]
    return high + [row - top for row, top in zip(entries, high)]


def fit_tables(day_ref, table_ref, edge_row, edge_lane):
    dates = day_ref.shape[1]
    width = 8 * dates
    day = jnp.broadcast_to(day_ref[...], (8, dates))
    digits = jnp.concatenate([day >> 4, day & 15], axis=0).astype(jnp.float32).astype(jnp.bfloat16)
    owner = lane_iota((dates, width), 1) // 8 == lane_iota((dates, width), 0)
    spread = jnp.dot(digits, jnp.where(owner, 1.0, 0.0).astype(jnp.bfloat16), preferred_element_type=jnp.float32)
    basis, months = fit_rows(16.0 * spread[:8] + spread[8:])
    products = [basis[i] * basis[j] for i in range(8) for j in range(i + 1)]
    diagonal = lane_iota((8, width), 1) % 8 == lane_iota((8, width), 0)
    short_basis, short_months = fit_rows(day.astype(jnp.float32))
    bottom = lane_iota((8, dates), 0) == 7
    for row0, lane0, keep, entries in (
        (0, 0, diagonal, two_parts(basis[1:]) + months),
        (TABLE, 0, diagonal, two_parts(products) + months),
        (edge_row, edge_lane, bottom, two_parts(short_basis[1:]) + short_months),
    ):
        for k in range(0, len(entries), 2):
            tile = jnp.concatenate([jnp.where(keep, row, 0.0) for row in entries[k : k + 2]], axis=0)
            table_ref[row0 + 8 * k : row0 + 8 * k + 16, lane0 : lane0 + keep.shape[1]] = tile.astype(jnp.bfloat16)


def own_words(words, first, bits_ref, b8):
    cells_here, cols = b8.shape[1:]
    strips, lanes = cols // STRIP, bits_ref.shape[1]
    blocks = bits_ref.shape[0] // strips // words
    block, within = first // lanes, lax.rem(first, lanes)
    lane = lane_iota((strips, lanes), 1)
    joined = jnp.zeros((strips, lanes), jnp.int32)
    for w in range(words):
        word = bits_ref[pl.ds(blocks * w + block, strips, stride=blocks * words), :]
        word = jnp.where(lane < cells_here, pltpu.roll(word, lax.rem(lanes - within, lanes), 1), 0)
        copies = word | pltpu.roll(word, cells_here, 1)
        copies = copies | pltpu.roll(copies, 2 * cells_here, 1)
        joined = joined | (pltpu.roll(copies, 4 * cells_here * w, 1) if w else copies)
    digits = lax.shift_right_logical(joined, 8 * (lane // cells_here % 4)) & 255
    mine = lane_iota((strips, cols), 1) // STRIP == lane_iota((strips, cols), 0)
    spread = lax.dot_general(
        digits.astype(jnp.float32).astype(jnp.bfloat16),
        jnp.where(mine, 1.0, 0.0).astype(jnp.bfloat16),
        (((0,), (0,)), ((), ())),
        preferred_element_type=jnp.float32,
    ).astype(jnp.int32)
    for w in range(words):
        parts = [spread[cells_here * (4 * w + k) : cells_here * (4 * w + k + 1)] << (8 * k) for k in range(4)]
        b8[w] = parts[0] | parts[1] | parts[2] | parts[3]


def solve_cells(g_ref, inv_ref):
    pairs = [(i, j) for i in range(8) for j in range(i + 1)]
    gram = {
        ij: g_ref[8 * n : 8 * n + 8] + g_ref[8 * (n + 36) : 8 * (n + 36) + 8] for n, ij in enumerate(pairs)
    }
    factor, root = {}, {}
    for j in range(8):
        root[j] = lax.rsqrt(gram[j, j] + RIDGE)
        for i in range(j + 1, 8):
            factor[i, j] = gram[i, j] * root[j]
        for k in range(j + 1, 8):
            for i in range(k, 8):
                gram[i, k] = gram[i, k] - factor[i, j] * factor[k, j]
    lower = {}
    for j in range(8):
        lower[j, j] = root[j]
        for i in range(j + 1, 8):
            running = factor[i, j] * lower[j, j]
            for k in range(j + 1, i):
                running = running + factor[i, k] * lower[k, j]
            lower[i, j] = -running * root[i]
    for n, (i, j) in enumerate(pairs):
        total = lower[i, i] * lower[i, j]
        for k in range(i + 1, 8):
            total = total + lower[k, i] * lower[k, j]
        inv_ref[n] = total
    counts = [g_ref[8 * (72 + m) : 8 * (72 + m) + 8] for m in range(12)]
    whole = counts[0]
    for m in range(1, 12):
        whole = whole + counts[m]
    for m in range(12):
        inv_ref[36 + m] = 1.0 / jnp.maximum(counts[m], 1.0)
    inv_ref[48] = 1.0 / jnp.maximum(whole, 1.0)


def resample_body(
    foot_far,
    offs_far,
    day_far,
    smooth_far,
    scene_far,
    x_far,
    table_far,
    foot_ref,
    offs_ref,
    day_ref,
    foot_rows,
    offs_rows,
    small_sem,
    scene,
    x_ref,
    table_ref,
    lines,
    in_sem,
    out_sem,
):
    f32, bf16 = jnp.float32, jnp.bfloat16
    dates, bands, rows, cols = scene.shape
    parts = rows // 8
    chunks = in_sem.shape[0] - 1
    chunk = dates // chunks
    table_rows, product_rows, width = TABLE, PRODUCT, table_ref.shape[1]
    smooth_row = table_rows + product_rows
    cover_row = smooth_row + 2 * cols

    def load(k):
        part = pl.ds(k * chunk, chunk)
        return pltpu.make_async_copy(scene_far.at[part], scene.at[part], in_sem.at[k])

    smooth = pltpu.make_async_copy(
        smooth_far, table_ref.at[pl.ds(smooth_row, 2 * cols), :], in_sem.at[chunks]
    )
    load(0).start()
    small = [
        pltpu.make_async_copy(far, near, small_sem.at[k])
        for k, (far, near) in enumerate(
            (
                (day_far, day_ref),
                (foot_far, foot_ref),
                (offs_far, offs_ref),
                (foot_far, foot_rows),
                (offs_far, offs_rows),
            )
        )
    ]
    for copy in small:
        copy.start()
    for k in range(1, chunks):
        load(k).start()
    smooth.start()
    for copy in small:
        copy.wait()

    table_ref[cover_row : cover_row + TABLE, 2 * cols : 3 * cols] = jnp.zeros((TABLE, cols), bf16)
    fit_tables(day_ref, table_ref, cover_row, 2 * cols)
    strip = lane_iota((8, cols), 1) // STRIP
    span = dates * 8 // 2
    lines[...] = jnp.zeros_like(lines)
    lines[0:2, :dates] = foot_rows[...].astype(f32)
    lines[2:4, :dates] = offs_rows[...].astype(f32) * (1.0 / 16.0)
    column = lines[...].T[:EDGES]
    first, last, fy, fx = (jnp.broadcast_to(column[:, k : k + 1], (EDGES, cols)) for k in range(4))
    lane = lane_iota((EDGES, cols), 1)
    here = (lane // STRIP).astype(f32)
    for k, entry in enumerate(
        (
            fy * (1.0 - fx),
            jnp.where(lane > 0, fy * fx, 0.0),
            jnp.where((here >= first) & (here <= last), 1.0, 0.0),
        )
    ):
        table_ref[cover_row + k * EDGES : cover_row + (k + 1) * EDGES, 3 * cols : 4 * cols] = entry.astype(bf16)

    for side in range(2):

        def cover(tp, carry, lane=side):
            tiles = []
            for u in (0, 1):
                t = lane * (span // 8) + 2 * tp + u
                inside = (strip >= foot_ref[0, t]) & (strip <= foot_ref[1, t])
                tiles.append(jnp.where(inside, 1.0, 0.0))
            row = pl.multiple_of(cover_row + 16 * tp, 16)
            table_ref[pl.ds(row, 16), lane * cols : (lane + 1) * cols] = jnp.concatenate(tiles, axis=0).astype(bf16)
            return carry

        lax.fori_loop(0, span // 16, cover, 0)
    used = cover_row + span
    smooth.wait()
    save_table = pltpu.make_async_copy(
        table_ref.at[pl.ds(0, used), :], table_far.at[pl.ds(0, used), :], out_sem.at[0]
    )
    save_table.start()

    not_last = lane_iota((8, cols), 1) < cols - 1
    bottom = lane_iota((8, cols), 0) == 7

    def splat(value):
        return jnp.full((8, cols), value, jnp.int32).astype(f32) * (1.0 / 16.0)

    def pair(tp, carry):
        fractions = []
        for u in (0, 1):
            t = 2 * tp + u
            fy, fx = splat(offs_ref[0, t]), splat(offs_ref[1, t])
            fractions.append((fy, 1.0 - fy, 1.0 - fx, jnp.where(not_last, fx, 0.0)))
        for s in range(bands):
            halves = []
            for u in (0, 1):
                fy, gy, keep, take = fractions[u]
                source = scene[2 * tp + u, s].astype(f32)
                across = []
                for part in range(parts):
                    piece = source[8 * part : 8 * part + 8]
                    across.append(keep * piece + take * pltpu.roll(piece, cols - 1, 1))
                turned = [pltpu.roll(piece, 7, 0) for piece in across]
                turned.append(0.0)
                halves.append(
                    [
                        gy * across[part] + fy * jnp.where(bottom, turned[part + 1], turned[part])
                        for part in range(parts)
                    ]
                )
            for part in range(parts):
                tile = jnp.concatenate([halves[0][part], halves[1][part]], axis=0)
                x_ref[part, s, pl.ds(pl.multiple_of(16 * tp, 16), 16), :] = tile.astype(bf16)
        return carry

    def save(k):
        inner = pl.ds(k * chunk * 8, chunk * 8)
        return pltpu.make_async_copy(x_ref.at[:, :, inner, :], x_far.at[:, :, inner, :], out_sem.at[1 + k])

    for k in range(chunks):
        load(k).wait()
        lax.fori_loop(k * chunk // 2, (k + 1) * chunk // 2, pair, 0)
        save(k).start()
    save_table.wait()
    for k in range(chunks):
        save(k).wait()


def fit_body(
    words,
    place_ref,
    bits_ref,
    below_ref,
    x_far,
    table_far,
    send_ref,
    x_ref,
    table_ref,
    below_wide,
    edge_ref,
    b8,
    bfull,
    wc_ref,
    w_ref,
    g_ref,
    inv_ref,
    wide_ref,
    y_ref,
    in_sem,
):
    f32, bf16 = jnp.float32, jnp.bfloat16
    dates, bands, cols = below_ref.shape
    cells_here = b8.shape[1]
    steps, _, _, wide = bfull.shape
    group = wide // cols
    parts = steps * group
    rows = 8 * parts
    half = cells_here // parts
    depth, width = 8 * dates, table_ref.shape[1]
    smooth_row = TABLE + PRODUCT
    cover_row = smooth_row + 2 * cols
    span = depth // words
    arrivals = [
        pltpu.make_async_copy(far, near, in_sem.at[k])
        for k, (far, near) in enumerate(
            (
                (table_far.at[pl.ds(cover_row, span), :], table_ref.at[pl.ds(cover_row, span), :]),
                (table_far.at[pl.ds(0, cover_row), :], table_ref.at[pl.ds(0, cover_row), :]),
                (x_far, x_ref),
            )
        )
    ]
    for copy in arrivals:
        copy.start()

    own_words(words, place_ref[0] * cells_here, bits_ref, b8)
    y_ref[...] = jnp.zeros_like(y_ref)
    top = lane_iota((8, cols), 0) < 8 // half
    for w in range(words):
        for part in range(parts):
            q, g = divmod(part, group)
            bfull[q, w, :, g * cols : (g + 1) * cols] = jnp.where(
                top, b8[w, part * half : part * half + 1, :], b8[w, part * half + 1 : part * half + 2, :]
            )

    def spread_rows(t, carry):
        below_wide[pl.ds(pl.multiple_of(8 * t, 8), bands), :] = below_ref[t].astype(f32)
        return carry

    lax.fori_loop(0, dates, spread_rows, 0)
    arrivals[0].wait()
    per_word = dates // words
    when = lane_iota((EDGES, cols), 0)
    word = b8[0, cells_here - 1 : cells_here, :]
    for w in range(1, words):
        word = jnp.where(when >= w * per_word, b8[w, cells_here - 1 : cells_here, :], word)
    flag = (lax.shift_right_logical(jnp.broadcast_to(word, (EDGES, cols)), when % per_word) & 1).astype(f32)
    near, far, cover = (
        table_ref[cover_row + k * EDGES : cover_row + (k + 1) * EDGES, 3 * cols : 4 * cols].astype(f32)
        for k in range(3)
    )
    flag = flag * cover
    near, far = near * flag, far
    for s in range(bands):
        row = below_wide[pl.ds(s, EDGES, stride=8), :]
        edge = near * row + flag * pltpu.roll(far * row, cols - 1, 1)
        edge_ref[s] = jnp.where(when < dates, edge, 0.0).astype(bf16)
    for lane in range(words):

        def mask_pair(tp, carry, lane=lane):
            cover = table_ref[pl.ds(pl.multiple_of(cover_row + 16 * tp, 16), 16), lane * cols : (lane + 1) * cols]
            first = lane * (span // 8) + 2 * tp
            w = first // per_word
            coarse = b8[w]
            fine = [bfull[q, w] for q in range(steps)]
            small, large = [], [[] for _ in range(steps)]
            for u in (0, 1):
                bit = jnp.left_shift(1, first + u - w * per_word)
                small.append(jnp.where((coarse & bit) != 0, 1.0, 0.0))
                for q in range(steps):
                    large[q].append(jnp.where((fine[q] & bit) != 0, 1.0, 0.0))
            row = pl.ds(pl.multiple_of(lane * span + 16 * tp, 16), 16)
            wc_ref[row, :] = jnp.concatenate(small, axis=0).astype(bf16) * cover
            for q in range(steps):
                both = jnp.concatenate(large[q], axis=0).astype(bf16)
                w_ref[q, row, :] = both * jnp.concatenate([cover] * group, axis=1)
            return carry

        lax.fori_loop(0, span // 16, mask_pair, 0)
    arrivals[1].wait()
    g_ref[...] = jnp.dot(table_ref[TABLE:smooth_row, :depth], wc_ref[...], preferred_element_type=f32)
    solve_cells(g_ref, inv_ref)

    def widen(block, carry):
        for k in range(7):
            n = 7 * block + k
            for part in range(parts):
                q, g = divmod(part, group)
                wide_ref[q, n, :, g * cols : (g + 1) * cols] = jnp.where(
                    top,
                    inv_ref[n, part * half : part * half + 1, :],
                    inv_ref[n, part * half + 1 : part * half + 2, :],
                )
        return carry

    lax.fori_loop(0, inv_ref.shape[0] // 7, widen, 0)

    arrivals[2].wait()

    coef_groups = cdiv(8 * bands, 16)
    order = {}
    for i in range(8):
        for j in range(i + 1):
            order[i, j] = order[j, i] = len(set(order.values()))

    def sums_of(q, s):
        weighted = jnp.concatenate([x_ref[q * group + g, s] for g in range(group)], axis=1) * w_ref[q]
        sums = jnp.dot(table_ref[:TABLE, :depth], weighted, preferred_element_type=f32)
        if q == steps - 1:
            edge = jnp.concatenate([jnp.zeros((EDGES, (group - 1) * cols), bf16), edge_ref[s]], axis=1)
            near_edge = table_ref[cover_row : cover_row + TABLE, 2 * cols : 2 * cols + EDGES]
            sums = sums + jnp.dot(near_edge, edge, preferred_element_type=f32)
        return sums

    def put(q, base, e, u, value):
        tall = jnp.concatenate([value[:, g * cols : (g + 1) * cols] for g in range(group)], axis=0)
        row = u % 8 * rows + q * group * 8
        y_ref[base + u // 8, row : row + group * 8, e * cols : (e + 1) * cols] = tall.astype(bf16)

    def use(q, s, sums):
        month = [sums[8 * (14 + m) : 8 * (14 + m) + 8] for m in range(12)]
        whole = month[0]
        for m in range(1, 12):
            whole = whole + month[m]
        rhs = [whole] + [sums[8 * k : 8 * k + 8] + sums[8 * (k + 7) : 8 * (k + 7) + 8] for k in range(7)]
        for m in range(12):
            put(q, coef_groups, m % 2, (m // 2) * bands + s, month[m] * wide_ref[q, 36 + m])
        put(q, coef_groups, s % 2, 6 * bands + s // 2, whole * wide_ref[q, 48])
        for i in range(8):
            value = wide_ref[q, order[i, 0]] * rhs[0]
            for j in range(1, 8):
                value = value + wide_ref[q, order[i, j]] * rhs[j]
            put(q, 0, i % 2, (i // 2) * bands + s, value)

    places = [(q, s) for q in range(steps) for s in range(bands)]
    waiting = sums_of(*places[0])
    for n, (q, s) in enumerate(places):
        ready = waiting
        if n + 1 < len(places):
            waiting = sums_of(*places[n + 1])
        use(q, s, ready)

    for at in range(y_ref.shape[0]):
        side = 0 if at < coef_groups else 2 * cols
        turned = lax.dot_general(
            table_ref[smooth_row:cover_row, side : side + 2 * cols],
            y_ref[at],
            (((1,), (1,)), ((), ())),
            preferred_element_type=f32,
        ).reshape(cols // STRIP, 2 * STRIP, 2 * cols)
        tile = jnp.concatenate([turned[:, :, :cols], turned[:, :, cols:]], axis=1)
        send_ref[:, 16 * at : 16 * at + 16, :] = tile.astype(bf16)


def finish_body(bands, recv_ref, coef_ref, month_ref, year_ref, field_ref, out_sem):
    strips, slots, lanes = recv_ref.shape
    groups = slots // 16
    coef_groups = cdiv(8 * bands, 16)
    quarter = lanes // 4
    lane = lane_iota((16, lanes), 1)
    low_half = lane < 2 * quarter
    even = lane // quarter % 2 == 0

    def save(k):
        first, count, target = (
            (0, 8 * bands, coef_ref),
            (8 * bands, 8 * bands, month_ref.at[pl.ds(0, 8 * bands)]),
            (16 * bands, 4 * bands, month_ref.at[pl.ds(8 * bands, 4 * bands)]),
            (20 * bands, bands, year_ref),
        )[k]
        return pltpu.make_async_copy(field_ref.at[pl.ds(first, count)], target, out_sem.at[k])

    def one_group(is_coef, at, carry):
        part = pl.ds(pl.multiple_of(16 * at, 16), 16)
        tiles = []
        for lt in range(strips // 4):
            x = [recv_ref[4 * lt + b, part, :] for b in range(4)]
            for b in (0, 1):
                first, second = x[b], x[b + 2]
                x[b] = jnp.where(low_half, first, pltpu.roll(second, 2 * quarter, 1))
                x[b + 2] = jnp.where(low_half, pltpu.roll(first, 2 * quarter, 1), second)
            for b in (0, 2):
                first, second = x[b], x[b + 1]
                x[b] = jnp.where(even, first, pltpu.roll(second, quarter, 1))
                x[b + 1] = jnp.where(even, pltpu.roll(first, 3 * quarter, 1), second)
            tiles.append(x)
        for p in range(4):
            field = jnp.concatenate([tile[p].astype(jnp.float32) for tile in tiles], axis=1)
            if not is_coef:
                full = field.shape[1]
                where = lane_iota(field.shape, 1)
                before = jnp.where(where == 0, 0.0, pltpu.roll(field, 1, 1))
                after = jnp.where(where == full - 1, 0.0, pltpu.roll(field, full - 1, 1))
                field = 0.25 * before + 0.5 * field + 0.25 * after
            for h in (0, 1):
                u = 8 * at + 4 * h + p
                late = u - 8 * coef_groups
                for e in (0, 1):
                    coef = (2 * (u // bands) + e) * bands + lax.rem(u, bands)
                    month = (2 * (late // bands) + e) * bands + lax.rem(late, bands)
                    mean = 2 * (late - 6 * bands) + e
                    v = coef if is_coef else jnp.where(late < 6 * bands, 8 * bands + month, 20 * bands + mean)
                    field_ref[v] = field[8 * h + 4 * e : 8 * h + 4 * e + 4]
        return carry

    lax.fori_loop(0, coef_groups, functools.partial(one_group, True), 0)
    save(0).start()
    early = coef_groups + 4 * bands // 8
    lax.fori_loop(coef_groups, early, functools.partial(one_group, False), 0)
    save(1).start()
    lax.fori_loop(early, groups, functools.partial(one_group, False), 0)
    save(2).start()
    save(3).start()
    for k in range(4):
        save(k).wait()


def turn_tables(strips, strip_width):
    cols = strips * strip_width
    row, col = np.arange(2 * cols)[:, None], np.arange(2 * cols)[None, :]
    column = strip_width * (row // (2 * strip_width)) + row % strip_width
    same = row // strip_width % 2 == col // cols
    apart = np.abs(column - col % cols)
    plain = np.where(same & (apart == 0), 1.0, 0.0)
    smooth = np.where(same, np.where(apart == 0, 0.5, np.where(apart == 1, 0.25, 0.0)), 0.0)
    return jnp.asarray(np.concatenate([plain, smooth], axis=1), jnp.bfloat16)


def whole_dates(scenes, clear_bits, footprint, offsets, acq_day):
    dates, bands, rows, cols = scenes.shape
    words, _, cells = clear_bits.shape
    strips = lax.axis_size("band")
    cells_here = cells // strips
    group, lanes, chunks = 2, 128, 6
    steps = rows // 8 // group
    depth, wide = 8 * dates, group * cols
    f32, bf16 = jnp.float32, jnp.bfloat16
    blocks = words * cells // lanes
    flags = jnp.broadcast_to(clear_bits.reshape(1, blocks, 1, lanes), (strips, blocks, 1, lanes))
    flags = lax.all_to_all(flags, "band", split_axis=0, concat_axis=0, tiled=True)
    below = shifted(scenes[:, :, 0, :], "band", -1)
    smem = pl.BlockSpec(memory_space=pltpu.SMEM)
    vmem = pl.BlockSpec(memory_space=pltpu.VMEM)
    anywhere = pl.BlockSpec(memory_space=pl.ANY)
    groups = cdiv(8 * bands, 16) + cdiv(13 * bands, 16)
    place = lax.axis_index("band").reshape(1).astype(jnp.int32)
    parts, table_width = rows // 8, 4 * cols
    x_shape = (parts, bands, depth, cols)
    table_shape = (TABLE + PRODUCT + 4 * cols + 16, table_width)
    resampled, table = pl.pallas_call(
        resample_body,
        in_specs=[anywhere] * 5,
        out_specs=[anywhere] * 2,
        out_shape=[
            jax.ShapeDtypeStruct(x_shape, bf16),
            jax.ShapeDtypeStruct(table_shape, bf16),
        ],
        scratch_shapes=[
            pltpu.SMEM((2, dates), jnp.int32),
            pltpu.SMEM((2, dates), jnp.int32),
            pltpu.VMEM((1, dates), jnp.int32),
            pltpu.VMEM((2, dates), jnp.int32),
            pltpu.VMEM((2, dates), jnp.int32),
            pltpu.SemaphoreType.DMA((5,)),
            pltpu.VMEM(scenes.shape, bf16),
            pltpu.VMEM(x_shape, bf16),
            pltpu.VMEM(table_shape, bf16),
            pltpu.VMEM((8, 128), f32),
            pltpu.SemaphoreType.DMA((chunks + 1,)),
            pltpu.SemaphoreType.DMA((chunks + 1,)),
        ],
        cost_estimate=pl.CostEstimate(flops=20_000_000, bytes_accessed=9_000_000, transcendentals=0),
        name="resample",
    )(footprint.T, offsets.T, acq_day.reshape(1, dates), turn_tables(strips, STRIP), scenes)
    send = pl.pallas_call(
        functools.partial(fit_body, words),
        in_specs=[smem, vmem, vmem, anywhere, anywhere],
        out_specs=vmem,
        out_shape=jax.ShapeDtypeStruct((strips, 16 * groups, 4 * rows), bf16),
        scratch_shapes=[
            pltpu.VMEM(x_shape, bf16),
            pltpu.VMEM(table_shape, bf16),
            pltpu.VMEM((8 * EDGES, cols), f32),
            pltpu.VMEM((bands, EDGES, cols), bf16),
            pltpu.VMEM((words, cells_here, cols), jnp.int32),
            pltpu.VMEM((steps, words, 8, wide), jnp.int32),
            pltpu.VMEM((depth, cols), bf16),
            pltpu.VMEM((steps, depth, wide), bf16),
            pltpu.VMEM((PRODUCT, cols), f32),
            pltpu.VMEM((49, cells_here, cols), f32),
            pltpu.VMEM((steps, 49, 8, wide), f32),
            pltpu.VMEM((groups, 8 * rows, 2 * cols), bf16),
            pltpu.SemaphoreType.DMA((3,)),
        ],
        compiler_params=pltpu.CompilerParams(vmem_limit_bytes=FIT_VMEM),
        cost_estimate=pl.CostEstimate(flops=20_000_000, bytes_accessed=6_000_000, transcendentals=0),
        name="fit",
    )(place, flags.reshape(strips * blocks, lanes), below, resampled, table)
    received = lax.all_to_all(send, "band", split_axis=0, concat_axis=0, tiled=True)
    row_count = rows * strips
    shapes = [(n * bands, STRIP, row_count) for n in (8, 12, 1)]
    coefficients, monthly, annual = pl.pallas_call(
        functools.partial(finish_body, bands),
        in_specs=[vmem],
        out_specs=[anywhere] * 3,
        out_shape=[jax.ShapeDtypeStruct(shape, f32) for shape in shapes],
        scratch_shapes=[
            pltpu.VMEM((16 * groups, STRIP, row_count), f32),
            pltpu.SemaphoreType.DMA((4,)),
        ],
        compiler_params=pltpu.CompilerParams(vmem_limit_bytes=8 << 20),
        name="finish",
    )(received)
    return (
        coefficients.reshape(8, bands, STRIP, row_count),
        monthly.reshape(12, bands, STRIP, row_count),
        annual,
    )


def shards(scenes, clear_bits, footprint, offsets, acq_day):
    dates, bands, rows, cols = scenes.shape
    strips = lax.axis_size("band")
    words, _, cells = clear_bits.shape
    whole = (
        lax.axis_size("tile") == 1
        and cols == 128
        and rows == 32
        and cols == STRIP * strips
        and cells == 8 * strips
        and words == 2
        and dates == 30 * words
        and dates % 12 == 0
        and dates <= 60
        and bands % 6 == 0
        and bands <= 6
    )
    plan = whole_dates if whole else split_dates
    return plan(scenes, clear_bits, footprint, offsets, acq_day)


def solution(mesh):
    placed = (
        P(("region", "tile"), "sub", "band", None),
        P(("region", "tile"), "band", None),
        P(("region", "tile"), None),
        P(("region", "tile"), None),
        P(("region", "tile")),
    )
    return jax.shard_map(
        shards,
        mesh=mesh,
        in_specs=placed,
        out_specs=(
            P("region", "sub", "band", "tile"),
            P(("region", "tile"), "sub", "band", None),
            P(("region", "sub"), "band", "tile"),
        ),
        check_vma=False,
    )
```

```python
import functools

import jax
import jax.numpy as jnp
import numpy as np
from jax import lax
from jax.experimental import pallas as pl
from jax.experimental.pallas import tpu as pltpu
from jax.sharding import PartitionSpec as P

RIDGE = 1.0
STRIP = 4
TABLE = 8 * 26
PRODUCT = 8 * 84
EDGES = 64
RESAMPLE_VMEM = 16 << 20
FIT_VMEM = 20 << 20


def shifted(value, axis, steps):
    count = lax.axis_size(axis)
    first, last = (max(0, -steps), min(count, count - steps))
    return lax.ppermute(value, axis, [(source, source + steps) for source in range(first, last)])


def extended(x, sides, width):
    for axis, dim in sides:
        devices, length = (lax.axis_size(axis), x.shape[dim])
        up = [(i, (i + 1) % devices) for i in range(devices - 1)]
        down = [(j, i) for i, j in up]
        last = lax.slice_in_dim(x, length - width, length, axis=dim)
        first = lax.slice_in_dim(x, 0, width, axis=dim)
        before = lax.ppermute(last, axis, up)
        after = lax.ppermute(first, axis, down)
        x = jnp.concatenate([before, x, after], axis=dim)
    return x


def design_tables(acq_day):
    day_phase = acq_day.astype(jnp.float32) / 365.0
    columns = [jnp.ones_like(day_phase), 2.0 * day_phase - 1.0]
    for harmonic in (1, 2, 3):
        turn_angle = 2.0 * jnp.pi * harmonic * day_phase
        columns = columns + [jnp.cos(turn_angle), jnp.sin(turn_angle)]
    harmonic_basis = jnp.stack(columns, axis=1)
    month_index = acq_day * 12 // 365
    onehot = (month_index[:, None] == jnp.arange(12, dtype=jnp.int32)[None, :]).astype(jnp.float32)
    products = jnp.stack(
        [
            harmonic_basis[:, row_term] * harmonic_basis[:, col_term]
            for row_term in range(8)
            for col_term in range(row_term + 1)
        ],
        axis=1,
    )
    return (
        jnp.concatenate([products, onehot], axis=1),
        jnp.concatenate([harmonic_basis, onehot], axis=1),
    )


def bilinear(padded, offsets):
    shift_row = (offsets[:, 0].astype(jnp.float32) / 16.0)[:, None, None, None]
    shift_col = (offsets[:, 1].astype(jnp.float32) / 16.0)[:, None, None, None]
    upper_rows = padded[:, :, :-1].astype(jnp.float32)
    lower_rows = padded[:, :, 1:].astype(jnp.float32)

    def across(source):
        right_cell = jnp.concatenate([source[..., 1:], jnp.zeros_like(source[..., :1])], axis=-1)
        return (1.0 - shift_col) * source + shift_col * right_cell

    return ((1.0 - shift_row) * across(upper_rows) + shift_row * across(lower_rows)).astype(
        jnp.bfloat16
    )


def clear_weight(cell_words, footprint, strip_width):
    date_count = footprint.shape[0]
    per_date = jnp.repeat(cell_words, 30, axis=0)
    bit_place = (jnp.arange(date_count, dtype=jnp.int32) % 30)[:, None, None]
    clear_flag = jnp.right_shift(per_date, bit_place) & 1
    pixel_flag = jnp.repeat(jnp.repeat(clear_flag, 4, axis=1), 4, axis=2)
    strip_index = jnp.arange(pixel_flag.shape[1], dtype=jnp.int32) // strip_width
    covered = (strip_index[None, :] >= footprint[:, 0:1]) & (
        strip_index[None, :] <= footprint[:, 1:2]
    )
    return pixel_flag.astype(jnp.float32) * covered[:, :, None].astype(jnp.float32)


def partial_sums(weight, values, common_table, banded_table):
    common = jnp.einsum("dxy,dk->kxy", weight, common_table, precision=lax.Precision.HIGHEST)
    weighted = values.astype(jnp.float32) * weight[:, None]
    banded = jnp.einsum("dsxy,dk->ksxy", weighted, banded_table, precision=lax.Precision.HIGHEST)
    return (common, banded)


def solve_normal(gram, rhs):
    pair_list = [(row_term, col_term) for row_term in range(8) for col_term in range(row_term + 1)]
    gram_entry = {}
    for position, term_pair in enumerate(pair_list):
        gram_entry[term_pair] = gram[position]
    factor = {}
    for col_term in range(8):
        pivot_value = gram_entry[col_term, col_term] + RIDGE
        for inner_term in range(col_term):
            pivot_value = pivot_value - factor[col_term, inner_term] * factor[col_term, inner_term]
        diag_root = jnp.sqrt(pivot_value)
        factor[col_term, col_term] = diag_root
        for row_term in range(col_term + 1, 8):
            running = gram_entry[row_term, col_term]
            for inner_term in range(col_term):
                running = running - factor[row_term, inner_term] * factor[col_term, inner_term]
            factor[row_term, col_term] = running / diag_root
    forward = []
    for row_term in range(8):
        running = rhs[row_term]
        for inner_term in range(row_term):
            running = running - factor[row_term, inner_term] * forward[inner_term]
        forward.append(running / factor[row_term, row_term])
    backward = [forward[0]] * 8
    for row_term in reversed(range(8)):
        running = forward[row_term]
        for inner_term in range(row_term + 1, 8):
            running = running - factor[inner_term, row_term] * backward[inner_term]
        backward[row_term] = running / factor[row_term, row_term]
    return jnp.stack(backward, axis=0)


def smooth_axis(padded_field, along):
    inner_size = padded_field.shape[along] - 2
    left_part = lax.slice_in_dim(padded_field, 0, inner_size, axis=along)
    centre_part = lax.slice_in_dim(padded_field, 1, inner_size + 1, axis=along)
    right_part = lax.slice_in_dim(padded_field, 2, inner_size + 2, axis=along)
    return 0.25 * left_part + 0.5 * centre_part + 0.25 * right_part


def split_dates(scenes, clear_bits, footprint, offsets, acq_day):
    date_count, band_count, row_local, col_count = scenes.shape
    strip_count = lax.axis_size("band")
    tile_count = lax.axis_size("tile")
    strip_width = col_count // strip_count
    row_count = row_local * strip_count
    common_table, banded_table = design_tables(acq_day)
    below = shifted(scenes[:, :, 0:1, :], "band", -1)
    resampled = bilinear(jnp.concatenate([scenes, below], axis=2), offsets)
    flipped = jnp.swapaxes(resampled, 2, 3)
    cell_words = lax.all_to_all(clear_bits, "band", split_axis=2, concat_axis=1, tiled=True)
    weight = clear_weight(cell_words, footprint, strip_width)
    common, banded = partial_sums(weight, flipped, common_table, banded_table)
    common, banded = (
        lax.all_to_all(common, "band", split_axis=1, concat_axis=2, tiled=True),
        lax.all_to_all(
            banded.reshape(-1, col_count, row_local),
            "band",
            split_axis=1,
            concat_axis=2,
            tiled=True,
        ),
    )
    banded = banded.reshape(20, band_count, strip_width, row_count)
    gram = common[:36]
    month_count = common[36:]
    rhs = banded[:8]
    month_sum = banded[8:]
    annual_sum = jnp.sum(month_sum, axis=0)
    annual_count = jnp.sum(month_count, axis=0)
    month_sum, month_count = (
        lax.psum_scatter(month_sum, "tile", scatter_dimension=0, tiled=True),
        lax.psum_scatter(month_count, "tile", scatter_dimension=0, tiled=True),
    )
    composite = month_sum / jnp.maximum(month_count, 1.0)[:, None]
    month_edged = extended(composite, (("band", 2),), 1)
    month_edged = jnp.pad(month_edged, ((0, 0), (0, 0), (0, 0), (1, 1)))
    monthly = smooth_axis(smooth_axis(month_edged, 3), 2)
    share = row_count // tile_count
    gram, rhs, annual_sum, annual_count = lax.psum((gram, rhs, annual_sum, annual_count), "tile")
    start = lax.axis_index("tile") * share
    gram = lax.dynamic_slice_in_dim(gram, start, share, 2)
    rhs = lax.dynamic_slice_in_dim(rhs, start, share, 3)
    annual_sum = lax.dynamic_slice_in_dim(annual_sum, start, share, 2)
    annual_count = lax.dynamic_slice_in_dim(annual_count, start, share, 1)
    coefficients = solve_normal(gram, rhs)
    yearly = annual_sum / jnp.maximum(annual_count, 1.0)
    year_edged = extended(yearly, (("band", 1), ("tile", 2)), 1)
    annual = smooth_axis(smooth_axis(year_edged, 2), 1)
    return (coefficients, monthly, annual)


def cdiv(a, b):
    return -(-a // b)


def lane_iota(shape, dim):
    return lax.broadcasted_iota(jnp.int32, shape, dim)


def fit_rows(day):
    phase = day / 365.0
    turn = 2.0 * jnp.pi * phase
    c, s = jnp.cos(turn), jnp.sin(turn)
    basis = [
        jnp.ones_like(phase),
        2.0 * phase - 1.0,
        c,
        s,
        2.0 * c * c - 1.0,
        2.0 * s * c,
        (4.0 * c * c - 3.0) * c,
        (3.0 - 4.0 * s * s) * s,
    ]
    months = [
        jnp.where((12.0 * day >= 365.0 * m) & (12.0 * day < 365.0 * (m + 1)), 1.0, 0.0) for m in range(12)
    ]
    return basis, months


def two_parts(entries):
    high = [row.astype(jnp.bfloat16).astype(jnp.float32) for row in entries]
    return high + [row - top for row, top in zip(entries, high)]


def fit_tables(day_ref, table_ref, edge_row, edge_lane):
    dates = day_ref.shape[1]
    width = 8 * dates
    day = jnp.broadcast_to(day_ref[...], (8, dates))
    digits = jnp.concatenate([day >> 4, day & 15], axis=0).astype(jnp.float32).astype(jnp.bfloat16)
    owner = lane_iota((dates, width), 1) // 8 == lane_iota((dates, width), 0)
    spread = jnp.dot(digits, jnp.where(owner, 1.0, 0.0).astype(jnp.bfloat16), preferred_element_type=jnp.float32)
    basis, months = fit_rows(16.0 * spread[:8] + spread[8:])
    products = [basis[i] * basis[j] for i in range(8) for j in range(i + 1)]
    diagonal = lane_iota((8, width), 1) % 8 == lane_iota((8, width), 0)
    short_basis, short_months = fit_rows(day.astype(jnp.float32))
    bottom = lane_iota((8, dates), 0) == 7
    for row0, lane0, keep, entries in (
        (0, 0, diagonal, two_parts(basis[1:]) + months),
        (TABLE, 0, diagonal, two_parts(products) + months),
        (edge_row, edge_lane, bottom, two_parts(short_basis[1:]) + short_months),
    ):
        for k in range(0, len(entries), 2):
            tile = jnp.concatenate([jnp.where(keep, row, 0.0) for row in entries[k : k + 2]], axis=0)
            table_ref[row0 + 8 * k : row0 + 8 * k + 16, lane0 : lane0 + keep.shape[1]] = tile.astype(jnp.bfloat16)


def own_words(words, first, bits_ref, b8):
    cells_here, cols = b8.shape[1:]
    strips, lanes = cols // STRIP, bits_ref.shape[1]
    blocks = bits_ref.shape[0] // strips // words
    block, within = first // lanes, lax.rem(first, lanes)
    lane = lane_iota((strips, lanes), 1)
    joined = jnp.zeros((strips, lanes), jnp.int32)
    for w in range(words):
        word = bits_ref[pl.ds(blocks * w + block, strips, stride=blocks * words), :]
        word = jnp.where(lane < cells_here, pltpu.roll(word, lax.rem(lanes - within, lanes), 1), 0)
        copies = word | pltpu.roll(word, cells_here, 1)
        copies = copies | pltpu.roll(copies, 2 * cells_here, 1)
        joined = joined | (pltpu.roll(copies, 4 * cells_here * w, 1) if w else copies)
    digits = lax.shift_right_logical(joined, 8 * (lane // cells_here % 4)) & 255
    mine = lane_iota((strips, cols), 1) // STRIP == lane_iota((strips, cols), 0)
    spread = lax.dot_general(
        digits.astype(jnp.float32).astype(jnp.bfloat16),
        jnp.where(mine, 1.0, 0.0).astype(jnp.bfloat16),
        (((0,), (0,)), ((), ())),
        preferred_element_type=jnp.float32,
    ).astype(jnp.int32)
    for w in range(words):
        parts = [spread[cells_here * (4 * w + k) : cells_here * (4 * w + k + 1)] << (8 * k) for k in range(4)]
        b8[w] = parts[0] | parts[1] | parts[2] | parts[3]


def solve_cells(g_ref, inv_ref):
    pairs = [(i, j) for i in range(8) for j in range(i + 1)]
    gram = {
        ij: g_ref[8 * n : 8 * n + 8] + g_ref[8 * (n + 36) : 8 * (n + 36) + 8] for n, ij in enumerate(pairs)
    }
    factor, root = {}, {}
    for j in range(8):
        root[j] = lax.rsqrt(gram[j, j] + RIDGE)
        for i in range(j + 1, 8):
            factor[i, j] = gram[i, j] * root[j]
        for k in range(j + 1, 8):
            for i in range(k, 8):
                gram[i, k] = gram[i, k] - factor[i, j] * factor[k, j]
    lower = {}
    for j in range(8):
        lower[j, j] = root[j]
        for i in range(j + 1, 8):
            running = factor[i, j] * lower[j, j]
            for k in range(j + 1, i):
                running = running + factor[i, k] * lower[k, j]
            lower[i, j] = -running * root[i]
    for n, (i, j) in enumerate(pairs):
        total = lower[i, i] * lower[i, j]
        for k in range(i + 1, 8):
            total = total + lower[k, i] * lower[k, j]
        inv_ref[n] = total
    counts = [g_ref[8 * (72 + m) : 8 * (72 + m) + 8] for m in range(12)]
    whole = counts[0]
    for m in range(1, 12):
        whole = whole + counts[m]
    for m in range(12):
        inv_ref[36 + m] = 1.0 / jnp.maximum(counts[m], 1.0)
    inv_ref[48] = 1.0 / jnp.maximum(whole, 1.0)


def resample_body(
    foot_far,
    offs_far,
    day_far,
    smooth_far,
    scene_far,
    x_ref,
    table_far,
    foot_ref,
    offs_ref,
    day_ref,
    foot_rows,
    offs_rows,
    small_sem,
    scene,
    table_ref,
    lines,
    in_sem,
    out_sem,
):
    f32, bf16 = jnp.float32, jnp.bfloat16
    dates, bands, rows, cols = scene.shape
    parts = rows // 8
    chunks = in_sem.shape[0] - 1
    chunk = dates // chunks
    table_rows, product_rows, width = TABLE, PRODUCT, table_ref.shape[1]
    smooth_row = table_rows + product_rows
    cover_row = smooth_row + 2 * cols

    def load(k):
        part = pl.ds(k * chunk, chunk)
        return pltpu.make_async_copy(scene_far.at[part], scene.at[part], in_sem.at[k])

    smooth = pltpu.make_async_copy(
        smooth_far, table_ref.at[pl.ds(smooth_row, 2 * cols), :], in_sem.at[chunks]
    )
    load(0).start()
    small = [
        pltpu.make_async_copy(far, near, small_sem.at[k])
        for k, (far, near) in enumerate(
            (
                (day_far, day_ref),
                (foot_far, foot_ref),
                (offs_far, offs_ref),
                (foot_far, foot_rows),
                (offs_far, offs_rows),
            )
        )
    ]
    for copy in small:
        copy.start()
    for k in range(1, chunks):
        load(k).start()
    smooth.start()
    for copy in small:
        copy.wait()

    table_ref[cover_row : cover_row + TABLE, 2 * cols : 3 * cols] = jnp.zeros((TABLE, cols), bf16)
    fit_tables(day_ref, table_ref, cover_row, 2 * cols)
    strip = lane_iota((8, cols), 1) // STRIP
    span = dates * 8 // 2
    lines[...] = jnp.zeros_like(lines)
    lines[0:2, :dates] = foot_rows[...].astype(f32)
    lines[2:4, :dates] = offs_rows[...].astype(f32) * (1.0 / 16.0)
    column = lines[...].T[:EDGES]
    first, last, fy, fx = (jnp.broadcast_to(column[:, k : k + 1], (EDGES, cols)) for k in range(4))
    lane = lane_iota((EDGES, cols), 1)
    here = (lane // STRIP).astype(f32)
    for k, entry in enumerate(
        (
            fy * (1.0 - fx),
            jnp.where(lane > 0, fy * fx, 0.0),
            jnp.where((here >= first) & (here <= last), 1.0, 0.0),
        )
    ):
        table_ref[cover_row + k * EDGES : cover_row + (k + 1) * EDGES, 3 * cols : 4 * cols] = entry.astype(bf16)

    for side in range(2):

        def cover(tp, carry, lane=side):
            tiles = []
            for u in (0, 1):
                t = lane * (span // 8) + 2 * tp + u
                inside = (strip >= foot_ref[0, t]) & (strip <= foot_ref[1, t])
                tiles.append(jnp.where(inside, 1.0, 0.0))
            row = pl.multiple_of(cover_row + 16 * tp, 16)
            table_ref[pl.ds(row, 16), lane * cols : (lane + 1) * cols] = jnp.concatenate(tiles, axis=0).astype(bf16)
            return carry

        lax.fori_loop(0, span // 16, cover, 0)
    used = cover_row + span
    smooth.wait()
    save_table = pltpu.make_async_copy(
        table_ref.at[pl.ds(0, used), :], table_far.at[pl.ds(0, used), :], out_sem.at[0]
    )
    save_table.start()

    not_last = lane_iota((8, cols), 1) < cols - 1
    bottom = lane_iota((8, cols), 0) == 7

    def splat(value):
        return jnp.full((8, cols), value, jnp.int32).astype(f32) * (1.0 / 16.0)

    def pair(tp, carry):
        fractions = []
        for u in (0, 1):
            t = 2 * tp + u
            fy, fx = splat(offs_ref[0, t]), splat(offs_ref[1, t])
            fractions.append((fy, 1.0 - fy, 1.0 - fx, jnp.where(not_last, fx, 0.0)))
        for s in range(bands):
            halves = []
            for u in (0, 1):
                fy, gy, keep, take = fractions[u]
                raw = scene[2 * tp + u, s]
                source = raw.astype(f32)
                beside = pltpu.roll(raw, cols - 1, 1).astype(f32)
                across = []
                for part in range(parts):
                    piece = source[8 * part : 8 * part + 8]
                    across.append(keep * piece + take * beside[8 * part : 8 * part + 8])
                turned = [pltpu.roll(piece, 7, 0) for piece in across]
                turned.append(0.0)
                halves.append(
                    [
                        gy * across[part] + fy * jnp.where(bottom, turned[part + 1], turned[part])
                        for part in range(parts)
                    ]
                )
            for part in range(parts):
                tile = jnp.concatenate([halves[0][part], halves[1][part]], axis=0)
                x_ref[part, s, pl.ds(pl.multiple_of(16 * tp, 16), 16), :] = tile.astype(bf16)
        return carry

    for k in range(chunks):
        load(k).wait()
        lax.fori_loop(k * chunk // 2, (k + 1) * chunk // 2, pair, 0)
    save_table.wait()


def fit_body(
    words,
    place_ref,
    bits_ref,
    below_ref,
    x_ref,
    table_far,
    send_ref,
    table_ref,
    below_wide,
    edge_ref,
    b8,
    bfull,
    wc_ref,
    w_ref,
    g_ref,
    inv_ref,
    wide_ref,
    y_ref,
    in_sem,
):
    f32, bf16 = jnp.float32, jnp.bfloat16
    dates, bands, cols = below_ref.shape
    cells_here = b8.shape[1]
    steps, _, _, wide = bfull.shape
    group = wide // cols
    parts = steps * group
    rows = 8 * parts
    half = cells_here // parts
    depth, width = 8 * dates, table_ref.shape[1]
    smooth_row = TABLE + PRODUCT
    cover_row = smooth_row + 2 * cols
    span = depth // words
    arrivals = [
        pltpu.make_async_copy(table_far.at[part, :], table_ref.at[part, :], in_sem.at[k])
        for k, part in enumerate((pl.ds(cover_row, span), pl.ds(0, cover_row)))
    ]
    for copy in arrivals:
        copy.start()

    own_words(words, place_ref[0] * cells_here, bits_ref, b8)
    y_ref[...] = jnp.zeros_like(y_ref)
    top = lane_iota((8, cols), 0) < 8 // half
    for w in range(words):
        for part in range(parts):
            q, g = divmod(part, group)
            bfull[q, w, :, g * cols : (g + 1) * cols] = jnp.where(
                top, b8[w, part * half : part * half + 1, :], b8[w, part * half + 1 : part * half + 2, :]
            )

    def spread_rows(t, carry):
        below_wide[pl.ds(pl.multiple_of(8 * t, 8), bands), :] = below_ref[t].astype(f32)
        return carry

    lax.fori_loop(0, dates, spread_rows, 0)
    arrivals[0].wait()
    per_word = dates // words
    when = lane_iota((EDGES, cols), 0)
    word = b8[0, cells_here - 1 : cells_here, :]
    for w in range(1, words):
        word = jnp.where(when >= w * per_word, b8[w, cells_here - 1 : cells_here, :], word)
    flag = (lax.shift_right_logical(jnp.broadcast_to(word, (EDGES, cols)), when % per_word) & 1).astype(f32)
    near, far, cover = (
        table_ref[cover_row + k * EDGES : cover_row + (k + 1) * EDGES, 3 * cols : 4 * cols].astype(f32)
        for k in range(3)
    )
    flag = flag * cover
    near, far = near * flag, far
    for s in range(bands):
        row = below_wide[pl.ds(s, EDGES, stride=8), :]
        edge = near * row + flag * pltpu.roll(far * row, cols - 1, 1)
        edge_ref[s] = jnp.where(when < dates, edge, 0.0).astype(bf16)
    for lane in range(words):

        def mask_pair(tp, carry, lane=lane):
            cover = table_ref[pl.ds(pl.multiple_of(cover_row + 16 * tp, 16), 16), lane * cols : (lane + 1) * cols]
            first = lane * (span // 8) + 2 * tp
            w = first // per_word
            coarse = b8[w]
            fine = [bfull[q, w] for q in range(steps)]
            small, large = [], [[] for _ in range(steps)]
            for u in (0, 1):
                bit = jnp.left_shift(1, first + u - w * per_word)
                small.append(jnp.where((coarse & bit) != 0, 1.0, 0.0))
                for q in range(steps):
                    large[q].append(jnp.where((fine[q] & bit) != 0, 1.0, 0.0))
            row = pl.ds(pl.multiple_of(lane * span + 16 * tp, 16), 16)
            wc_ref[row, :] = jnp.concatenate(small, axis=0).astype(bf16) * cover
            for q in range(steps):
                both = jnp.concatenate(large[q], axis=0).astype(bf16)
                w_ref[q, row, :] = both * jnp.concatenate([cover] * group, axis=1)
            return carry

        lax.fori_loop(0, span // 16, mask_pair, 0)
    arrivals[1].wait()
    g_ref[...] = jnp.dot(table_ref[TABLE:smooth_row, :depth], wc_ref[...], preferred_element_type=f32)
    solve_cells(g_ref, inv_ref)

    def widen(block, carry):
        for k in range(7):
            n = 7 * block + k
            for part in range(parts):
                q, g = divmod(part, group)
                wide_ref[q, n, :, g * cols : (g + 1) * cols] = jnp.where(
                    top,
                    inv_ref[n, part * half : part * half + 1, :],
                    inv_ref[n, part * half + 1 : part * half + 2, :],
                )
        return carry

    lax.fori_loop(0, inv_ref.shape[0] // 7, widen, 0)


    coef_groups = cdiv(8 * bands, 16)
    order = {}
    for i in range(8):
        for j in range(i + 1):
            order[i, j] = order[j, i] = len(set(order.values()))

    def sums_of(q, s):
        weighted = jnp.concatenate([x_ref[q * group + g, s] for g in range(group)], axis=1) * w_ref[q]
        sums = jnp.dot(table_ref[:TABLE, :depth], weighted, preferred_element_type=f32)
        if q == steps - 1:
            edge = jnp.concatenate([jnp.zeros((EDGES, (group - 1) * cols), bf16), edge_ref[s]], axis=1)
            near_edge = table_ref[cover_row : cover_row + TABLE, 2 * cols : 2 * cols + EDGES]
            sums = sums + jnp.dot(near_edge, edge, preferred_element_type=f32)
        return sums

    def put(q, base, e, u, value):
        tall = jnp.concatenate([value[:, g * cols : (g + 1) * cols] for g in range(group)], axis=0)
        row = u % 8 * rows + q * group * 8
        y_ref[base + u // 8, row : row + group * 8, e * cols : (e + 1) * cols] = tall.astype(bf16)

    def use(q, s, sums):
        month = [sums[8 * (14 + m) : 8 * (14 + m) + 8] for m in range(12)]
        whole = month[0]
        for m in range(1, 12):
            whole = whole + month[m]
        rhs = [whole] + [sums[8 * k : 8 * k + 8] + sums[8 * (k + 7) : 8 * (k + 7) + 8] for k in range(7)]
        for m in range(12):
            put(q, coef_groups, m % 2, (m // 2) * bands + s, month[m] * wide_ref[q, 36 + m])
        put(q, coef_groups, s % 2, 6 * bands + s // 2, whole * wide_ref[q, 48])
        for i in range(8):
            value = wide_ref[q, order[i, 0]] * rhs[0]
            for j in range(1, 8):
                value = value + wide_ref[q, order[i, j]] * rhs[j]
            put(q, 0, i % 2, (i // 2) * bands + s, value)

    places = [(q, s) for q in range(steps) for s in range(bands)]
    waiting = sums_of(*places[0])
    for n, (q, s) in enumerate(places):
        ready = waiting
        if n + 1 < len(places):
            waiting = sums_of(*places[n + 1])
        use(q, s, ready)

    for at in range(y_ref.shape[0]):
        side = 0 if at < coef_groups else 2 * cols
        turned = lax.dot_general(
            table_ref[smooth_row:cover_row, side : side + 2 * cols],
            y_ref[at],
            (((1,), (1,)), ((), ())),
            preferred_element_type=f32,
        ).reshape(cols // STRIP, 2 * STRIP, 2 * cols)
        tile = jnp.concatenate([turned[:, :, :cols], turned[:, :, cols:]], axis=1)
        send_ref[:, 16 * at : 16 * at + 16, :] = tile.astype(bf16)


def finish_body(bands, recv_ref, coef_ref, month_ref, year_ref, field_ref, out_sem):
    strips, slots, lanes = recv_ref.shape
    groups = slots // 16
    coef_groups = cdiv(8 * bands, 16)
    quarter = lanes // 4
    lane = lane_iota((16, lanes), 1)
    low_half = lane < 2 * quarter
    even = lane // quarter % 2 == 0

    def save(k):
        first, count, target = (
            (0, 8 * bands, coef_ref),
            (8 * bands, 8 * bands, month_ref.at[pl.ds(0, 8 * bands)]),
            (16 * bands, 4 * bands, month_ref.at[pl.ds(8 * bands, 4 * bands)]),
            (20 * bands, bands, year_ref),
        )[k]
        return pltpu.make_async_copy(field_ref.at[pl.ds(first, count)], target, out_sem.at[k])

    def one_group(is_coef, at, carry):
        part = pl.ds(pl.multiple_of(16 * at, 16), 16)
        tiles = []
        for lt in range(strips // 4):
            x = [recv_ref[4 * lt + b, part, :] for b in range(4)]
            for b in (0, 1):
                first, second = x[b], x[b + 2]
                x[b] = jnp.where(low_half, first, pltpu.roll(second, 2 * quarter, 1))
                x[b + 2] = jnp.where(low_half, pltpu.roll(first, 2 * quarter, 1), second)
            for b in (0, 2):
                first, second = x[b], x[b + 1]
                x[b] = jnp.where(even, first, pltpu.roll(second, quarter, 1))
                x[b + 1] = jnp.where(even, pltpu.roll(first, 3 * quarter, 1), second)
            tiles.append(x)
        for p in range(4):
            field = jnp.concatenate([tile[p].astype(jnp.float32) for tile in tiles], axis=1)
            if not is_coef:
                full = field.shape[1]
                where = lane_iota(field.shape, 1)
                before = jnp.where(where == 0, 0.0, pltpu.roll(field, 1, 1))
                after = jnp.where(where == full - 1, 0.0, pltpu.roll(field, full - 1, 1))
                field = 0.25 * before + 0.5 * field + 0.25 * after
            for h in (0, 1):
                u = 8 * at + 4 * h + p
                late = u - 8 * coef_groups
                for e in (0, 1):
                    coef = (2 * (u // bands) + e) * bands + lax.rem(u, bands)
                    month = (2 * (late // bands) + e) * bands + lax.rem(late, bands)
                    mean = 2 * (late - 6 * bands) + e
                    v = coef if is_coef else jnp.where(late < 6 * bands, 8 * bands + month, 20 * bands + mean)
                    field_ref[v] = field[8 * h + 4 * e : 8 * h + 4 * e + 4]
        return carry

    lax.fori_loop(0, coef_groups, functools.partial(one_group, True), 0)
    save(0).start()
    early = coef_groups + 4 * bands // 8
    lax.fori_loop(coef_groups, early, functools.partial(one_group, False), 0)
    save(1).start()
    lax.fori_loop(early, groups, functools.partial(one_group, False), 0)
    save(2).start()
    save(3).start()
    for k in range(4):
        save(k).wait()


def turn_tables(strips, strip_width):
    cols = strips * strip_width
    row, col = np.arange(2 * cols)[:, None], np.arange(2 * cols)[None, :]
    column = strip_width * (row // (2 * strip_width)) + row % strip_width
    same = row // strip_width % 2 == col // cols
    apart = np.abs(column - col % cols)
    plain = np.where(same & (apart == 0), 1.0, 0.0)
    smooth = np.where(same, np.where(apart == 0, 0.5, np.where(apart == 1, 0.25, 0.0)), 0.0)
    return jnp.asarray(np.concatenate([plain, smooth], axis=1), jnp.bfloat16)


def whole_dates(scenes, clear_bits, footprint, offsets, acq_day):
    dates, bands, rows, cols = scenes.shape
    words, _, cells = clear_bits.shape
    strips = lax.axis_size("band")
    cells_here = cells // strips
    group, lanes, chunks = 2, 128, 3
    steps = rows // 8 // group
    depth, wide = 8 * dates, group * cols
    f32, bf16 = jnp.float32, jnp.bfloat16
    blocks = words * cells // lanes
    flags = jnp.broadcast_to(clear_bits.reshape(1, blocks, 1, lanes), (strips, blocks, 1, lanes))
    flags = lax.all_to_all(flags, "band", split_axis=0, concat_axis=0, tiled=True)
    below = shifted(scenes[:, :, 0, :], "band", -1)
    smem = pl.BlockSpec(memory_space=pltpu.SMEM)
    vmem = pl.BlockSpec(memory_space=pltpu.VMEM)
    anywhere = pl.BlockSpec(memory_space=pl.ANY)
    far = pl.BlockSpec(memory_space=pltpu.HBM)
    groups = cdiv(8 * bands, 16) + cdiv(13 * bands, 16)
    place = lax.axis_index("band").reshape(1).astype(jnp.int32)
    parts, table_width = rows // 8, 4 * cols
    x_shape = (parts, bands, depth, cols)
    table_shape = (TABLE + PRODUCT + 4 * cols + 16, table_width)
    def pinned(x):
        return pltpu.with_memory_space_constraint(x, pltpu.HBM)

    resampled, table = pl.pallas_call(
        resample_body,
        in_specs=[far] * 5,
        out_specs=[vmem, far],
        out_shape=[
            jax.ShapeDtypeStruct(x_shape, bf16),
            pltpu.HBM(table_shape, bf16),
        ],
        scratch_shapes=[
            pltpu.SMEM((2, dates), jnp.int32),
            pltpu.SMEM((2, dates), jnp.int32),
            pltpu.VMEM((1, dates), jnp.int32),
            pltpu.VMEM((2, dates), jnp.int32),
            pltpu.VMEM((2, dates), jnp.int32),
            pltpu.SemaphoreType.DMA((5,)),
            pltpu.VMEM(scenes.shape, bf16),
            pltpu.VMEM(table_shape, bf16),
            pltpu.VMEM((8, 128), f32),
            pltpu.SemaphoreType.DMA((chunks + 1,)),
            pltpu.SemaphoreType.DMA((1,)),
        ],
        compiler_params=pltpu.CompilerParams(vmem_limit_bytes=RESAMPLE_VMEM),
        cost_estimate=pl.CostEstimate(flops=20_000_000, bytes_accessed=9_000_000, transcendentals=0),
        name="resample",
    )(*(pinned(x) for x in (footprint.T, offsets.T, acq_day.reshape(1, dates), turn_tables(strips, STRIP), scenes)))
    send = pl.pallas_call(
        functools.partial(fit_body, words),
        in_specs=[smem, vmem, vmem, vmem, far],
        out_specs=vmem,
        out_shape=jax.ShapeDtypeStruct((strips, 16 * groups, 4 * rows), bf16),
        scratch_shapes=[
            pltpu.VMEM(table_shape, bf16),
            pltpu.VMEM((8 * EDGES, cols), f32),
            pltpu.VMEM((bands, EDGES, cols), bf16),
            pltpu.VMEM((words, cells_here, cols), jnp.int32),
            pltpu.VMEM((steps, words, 8, wide), jnp.int32),
            pltpu.VMEM((depth, cols), bf16),
            pltpu.VMEM((steps, depth, wide), bf16),
            pltpu.VMEM((PRODUCT, cols), f32),
            pltpu.VMEM((49, cells_here, cols), f32),
            pltpu.VMEM((steps, 49, 8, wide), f32),
            pltpu.VMEM((groups, 8 * rows, 2 * cols), bf16),
            pltpu.SemaphoreType.DMA((2,)),
        ],
        compiler_params=pltpu.CompilerParams(vmem_limit_bytes=FIT_VMEM),
        cost_estimate=pl.CostEstimate(flops=20_000_000, bytes_accessed=6_000_000, transcendentals=0),
        name="fit",
    )(place, flags.reshape(strips * blocks, lanes), below, resampled, pinned(table))
    received = lax.all_to_all(send, "band", split_axis=0, concat_axis=0, tiled=True)
    row_count = rows * strips
    shapes = [(n * bands, STRIP, row_count) for n in (8, 12, 1)]
    coefficients, monthly, annual = pl.pallas_call(
        functools.partial(finish_body, bands),
        in_specs=[vmem],
        out_specs=[anywhere] * 3,
        out_shape=[jax.ShapeDtypeStruct(shape, f32) for shape in shapes],
        scratch_shapes=[
            pltpu.VMEM((16 * groups, STRIP, row_count), f32),
            pltpu.SemaphoreType.DMA((4,)),
        ],
        compiler_params=pltpu.CompilerParams(vmem_limit_bytes=8 << 20),
        name="finish",
    )(received)
    return (
        coefficients.reshape(8, bands, STRIP, row_count),
        monthly.reshape(12, bands, STRIP, row_count),
        annual,
    )


def shards(scenes, clear_bits, footprint, offsets, acq_day):
    dates, bands, rows, cols = scenes.shape
    strips = lax.axis_size("band")
    words, _, cells = clear_bits.shape
    whole = (
        lax.axis_size("tile") == 1
        and cols == 128
        and rows == 32
        and cols == STRIP * strips
        and cells == 8 * strips
        and words == 2
        and dates == 30 * words
        and dates % 12 == 0
        and dates <= 60
        and bands % 6 == 0
        and bands <= 6
    )
    plan = whole_dates if whole else split_dates
    return plan(scenes, clear_bits, footprint, offsets, acq_day)


def solution(mesh):
    placed = (
        P(("region", "tile"), "sub", "band", None),
        P(("region", "tile"), "band", None),
        P(("region", "tile"), None),
        P(("region", "tile"), None),
        P(("region", "tile")),
    )
    return jax.shard_map(
        shards,
        mesh=mesh,
        in_specs=placed,
        out_specs=(
            P("region", "sub", "band", "tile"),
            P(("region", "tile"), "sub", "band", None),
            P(("region", "sub"), "band", "tile"),
        ),
        check_vma=False,
    )
```

```python
import functools

import jax
import jax.numpy as jnp
import numpy as np
from jax import lax
from jax.experimental import pallas as pl
from jax.experimental.pallas import tpu as pltpu
from jax.sharding import PartitionSpec as P

RIDGE = 1.0
STRIP = 4
TABLE = 8 * 26
PRODUCT = 8 * 84
EDGES = 64
RESAMPLE_VMEM = 16 << 20
FIT_VMEM = 20 << 20


def shifted(value, axis, steps):
    count = lax.axis_size(axis)
    first, last = (max(0, -steps), min(count, count - steps))
    return lax.ppermute(value, axis, [(source, source + steps) for source in range(first, last)])


def extended(x, sides, width):
    for axis, dim in sides:
        devices, length = (lax.axis_size(axis), x.shape[dim])
        up = [(i, (i + 1) % devices) for i in range(devices - 1)]
        down = [(j, i) for i, j in up]
        last = lax.slice_in_dim(x, length - width, length, axis=dim)
        first = lax.slice_in_dim(x, 0, width, axis=dim)
        before = lax.ppermute(last, axis, up)
        after = lax.ppermute(first, axis, down)
        x = jnp.concatenate([before, x, after], axis=dim)
    return x


def design_tables(acq_day):
    day_phase = acq_day.astype(jnp.float32) / 365.0
    columns = [jnp.ones_like(day_phase), 2.0 * day_phase - 1.0]
    for harmonic in (1, 2, 3):
        turn_angle = 2.0 * jnp.pi * harmonic * day_phase
        columns = columns + [jnp.cos(turn_angle), jnp.sin(turn_angle)]
    harmonic_basis = jnp.stack(columns, axis=1)
    month_index = acq_day * 12 // 365
    onehot = (month_index[:, None] == jnp.arange(12, dtype=jnp.int32)[None, :]).astype(jnp.float32)
    products = jnp.stack(
        [
            harmonic_basis[:, row_term] * harmonic_basis[:, col_term]
            for row_term in range(8)
            for col_term in range(row_term + 1)
        ],
        axis=1,
    )
    return (
        jnp.concatenate([products, onehot], axis=1),
        jnp.concatenate([harmonic_basis, onehot], axis=1),
    )


def bilinear(padded, offsets):
    shift_row = (offsets[:, 0].astype(jnp.float32) / 16.0)[:, None, None, None]
    shift_col = (offsets[:, 1].astype(jnp.float32) / 16.0)[:, None, None, None]
    upper_rows = padded[:, :, :-1].astype(jnp.float32)
    lower_rows = padded[:, :, 1:].astype(jnp.float32)

    def across(source):
        right_cell = jnp.concatenate([source[..., 1:], jnp.zeros_like(source[..., :1])], axis=-1)
        return (1.0 - shift_col) * source + shift_col * right_cell

    return ((1.0 - shift_row) * across(upper_rows) + shift_row * across(lower_rows)).astype(
        jnp.bfloat16
    )


def clear_weight(cell_words, footprint, strip_width):
    date_count = footprint.shape[0]
    per_date = jnp.repeat(cell_words, 30, axis=0)
    bit_place = (jnp.arange(date_count, dtype=jnp.int32) % 30)[:, None, None]
    clear_flag = jnp.right_shift(per_date, bit_place) & 1
    pixel_flag = jnp.repeat(jnp.repeat(clear_flag, 4, axis=1), 4, axis=2)
    strip_index = jnp.arange(pixel_flag.shape[1], dtype=jnp.int32) // strip_width
    covered = (strip_index[None, :] >= footprint[:, 0:1]) & (
        strip_index[None, :] <= footprint[:, 1:2]
    )
    return pixel_flag.astype(jnp.float32) * covered[:, :, None].astype(jnp.float32)


def partial_sums(weight, values, common_table, banded_table):
    common = jnp.einsum("dxy,dk->kxy", weight, common_table, precision=lax.Precision.HIGHEST)
    weighted = values.astype(jnp.float32) * weight[:, None]
    banded = jnp.einsum("dsxy,dk->ksxy", weighted, banded_table, precision=lax.Precision.HIGHEST)
    return (common, banded)


def solve_normal(gram, rhs):
    pair_list = [(row_term, col_term) for row_term in range(8) for col_term in range(row_term + 1)]
    gram_entry = {}
    for position, term_pair in enumerate(pair_list):
        gram_entry[term_pair] = gram[position]
    factor = {}
    for col_term in range(8):
        pivot_value = gram_entry[col_term, col_term] + RIDGE
        for inner_term in range(col_term):
            pivot_value = pivot_value - factor[col_term, inner_term] * factor[col_term, inner_term]
        diag_root = jnp.sqrt(pivot_value)
        factor[col_term, col_term] = diag_root
        for row_term in range(col_term + 1, 8):
            running = gram_entry[row_term, col_term]
            for inner_term in range(col_term):
                running = running - factor[row_term, inner_term] * factor[col_term, inner_term]
            factor[row_term, col_term] = running / diag_root
    forward = []
    for row_term in range(8):
        running = rhs[row_term]
        for inner_term in range(row_term):
            running = running - factor[row_term, inner_term] * forward[inner_term]
        forward.append(running / factor[row_term, row_term])
    backward = [forward[0]] * 8
    for row_term in reversed(range(8)):
        running = forward[row_term]
        for inner_term in range(row_term + 1, 8):
            running = running - factor[inner_term, row_term] * backward[inner_term]
        backward[row_term] = running / factor[row_term, row_term]
    return jnp.stack(backward, axis=0)


def smooth_axis(padded_field, along):
    inner_size = padded_field.shape[along] - 2
    left_part = lax.slice_in_dim(padded_field, 0, inner_size, axis=along)
    centre_part = lax.slice_in_dim(padded_field, 1, inner_size + 1, axis=along)
    right_part = lax.slice_in_dim(padded_field, 2, inner_size + 2, axis=along)
    return 0.25 * left_part + 0.5 * centre_part + 0.25 * right_part


def split_dates(scenes, clear_bits, footprint, offsets, acq_day):
    date_count, band_count, row_local, col_count = scenes.shape
    strip_count = lax.axis_size("band")
    tile_count = lax.axis_size("tile")
    strip_width = col_count // strip_count
    row_count = row_local * strip_count
    common_table, banded_table = design_tables(acq_day)
    below = shifted(scenes[:, :, 0:1, :], "band", -1)
    resampled = bilinear(jnp.concatenate([scenes, below], axis=2), offsets)
    flipped = jnp.swapaxes(resampled, 2, 3)
    cell_words = lax.all_to_all(clear_bits, "band", split_axis=2, concat_axis=1, tiled=True)
    weight = clear_weight(cell_words, footprint, strip_width)
    common, banded = partial_sums(weight, flipped, common_table, banded_table)
    common, banded = (
        lax.all_to_all(common, "band", split_axis=1, concat_axis=2, tiled=True),
        lax.all_to_all(
            banded.reshape(-1, col_count, row_local),
            "band",
            split_axis=1,
            concat_axis=2,
            tiled=True,
        ),
    )
    banded = banded.reshape(20, band_count, strip_width, row_count)
    gram = common[:36]
    month_count = common[36:]
    rhs = banded[:8]
    month_sum = banded[8:]
    annual_sum = jnp.sum(month_sum, axis=0)
    annual_count = jnp.sum(month_count, axis=0)
    month_sum, month_count = (
        lax.psum_scatter(month_sum, "tile", scatter_dimension=0, tiled=True),
        lax.psum_scatter(month_count, "tile", scatter_dimension=0, tiled=True),
    )
    composite = month_sum / jnp.maximum(month_count, 1.0)[:, None]
    month_edged = extended(composite, (("band", 2),), 1)
    month_edged = jnp.pad(month_edged, ((0, 0), (0, 0), (0, 0), (1, 1)))
    monthly = smooth_axis(smooth_axis(month_edged, 3), 2)
    share = row_count // tile_count
    gram, rhs, annual_sum, annual_count = lax.psum((gram, rhs, annual_sum, annual_count), "tile")
    start = lax.axis_index("tile") * share
    gram = lax.dynamic_slice_in_dim(gram, start, share, 2)
    rhs = lax.dynamic_slice_in_dim(rhs, start, share, 3)
    annual_sum = lax.dynamic_slice_in_dim(annual_sum, start, share, 2)
    annual_count = lax.dynamic_slice_in_dim(annual_count, start, share, 1)
    coefficients = solve_normal(gram, rhs)
    yearly = annual_sum / jnp.maximum(annual_count, 1.0)
    year_edged = extended(yearly, (("band", 1), ("tile", 2)), 1)
    annual = smooth_axis(smooth_axis(year_edged, 2), 1)
    return (coefficients, monthly, annual)


def cdiv(a, b):
    return -(-a // b)


def lane_iota(shape, dim):
    return lax.broadcasted_iota(jnp.int32, shape, dim)


def fit_rows(day):
    phase = day / 365.0
    turn = 2.0 * jnp.pi * phase
    c, s = jnp.cos(turn), jnp.sin(turn)
    basis = [
        jnp.ones_like(phase),
        2.0 * phase - 1.0,
        c,
        s,
        2.0 * c * c - 1.0,
        2.0 * s * c,
        (4.0 * c * c - 3.0) * c,
        (3.0 - 4.0 * s * s) * s,
    ]
    months = [
        jnp.where((12.0 * day >= 365.0 * m) & (12.0 * day < 365.0 * (m + 1)), 1.0, 0.0) for m in range(12)
    ]
    return basis, months


def two_parts(entries):
    high = [row.astype(jnp.bfloat16).astype(jnp.float32) for row in entries]
    return high + [row - top for row, top in zip(entries, high)]


def fit_tables(day_ref, table_ref, edge_row, edge_lane):
    dates = day_ref.shape[1]
    width = 8 * dates
    day = jnp.broadcast_to(day_ref[...], (8, dates))
    digits = jnp.concatenate([day >> 4, day & 15], axis=0).astype(jnp.float32).astype(jnp.bfloat16)
    owner = lane_iota((dates, width), 1) // 8 == lane_iota((dates, width), 0)
    spread = jnp.dot(digits, jnp.where(owner, 1.0, 0.0).astype(jnp.bfloat16), preferred_element_type=jnp.float32)
    basis, months = fit_rows(16.0 * spread[:8] + spread[8:])
    products = [basis[i] * basis[j] for i in range(8) for j in range(i + 1)]
    diagonal = lane_iota((8, width), 1) % 8 == lane_iota((8, width), 0)
    short_basis, short_months = fit_rows(day.astype(jnp.float32))
    bottom = lane_iota((8, dates), 0) == 7
    for row0, lane0, keep, entries in (
        (0, 0, diagonal, two_parts(basis[1:]) + months),
        (TABLE, 0, diagonal, two_parts(products) + months),
        (edge_row, edge_lane, bottom, two_parts(short_basis[1:]) + short_months),
    ):
        for k in range(0, len(entries), 2):
            tile = jnp.concatenate([jnp.where(keep, row, 0.0) for row in entries[k : k + 2]], axis=0)
            table_ref[row0 + 8 * k : row0 + 8 * k + 16, lane0 : lane0 + keep.shape[1]] = tile.astype(jnp.bfloat16)


def own_words(words, first, bits_ref, b8):
    cells_here, cols = b8.shape[1:]
    strips, lanes = cols // STRIP, bits_ref.shape[1]
    blocks = bits_ref.shape[0] // strips // words
    block, within = first // lanes, lax.rem(first, lanes)
    lane = lane_iota((strips, lanes), 1)
    joined = jnp.zeros((strips, lanes), jnp.int32)
    for w in range(words):
        word = bits_ref[pl.ds(blocks * w + block, strips, stride=blocks * words), :]
        word = jnp.where(lane < cells_here, pltpu.roll(word, lax.rem(lanes - within, lanes), 1), 0)
        copies = word | pltpu.roll(word, cells_here, 1)
        copies = copies | pltpu.roll(copies, 2 * cells_here, 1)
        joined = joined | (pltpu.roll(copies, 4 * cells_here * w, 1) if w else copies)
    digits = lax.shift_right_logical(joined, 8 * (lane // cells_here % 4)) & 255
    mine = lane_iota((strips, cols), 1) // STRIP == lane_iota((strips, cols), 0)
    spread = lax.dot_general(
        digits.astype(jnp.float32).astype(jnp.bfloat16),
        jnp.where(mine, 1.0, 0.0).astype(jnp.bfloat16),
        (((0,), (0,)), ((), ())),
        preferred_element_type=jnp.float32,
    ).astype(jnp.int32)
    for w in range(words):
        parts = [spread[cells_here * (4 * w + k) : cells_here * (4 * w + k + 1)] << (8 * k) for k in range(4)]
        b8[w] = parts[0] | parts[1] | parts[2] | parts[3]


def solve_cells(g_ref, inv_ref):
    pairs = [(i, j) for i in range(8) for j in range(i + 1)]
    gram = {
        ij: g_ref[8 * n : 8 * n + 8] + g_ref[8 * (n + 36) : 8 * (n + 36) + 8] for n, ij in enumerate(pairs)
    }
    factor, root = {}, {}
    for j in range(8):
        root[j] = lax.rsqrt(gram[j, j] + RIDGE)
        for i in range(j + 1, 8):
            factor[i, j] = gram[i, j] * root[j]
        for k in range(j + 1, 8):
            for i in range(k, 8):
                gram[i, k] = gram[i, k] - factor[i, j] * factor[k, j]
    lower = {}
    for j in range(8):
        lower[j, j] = root[j]
        for i in range(j + 1, 8):
            running = factor[i, j] * lower[j, j]
            for k in range(j + 1, i):
                running = running + factor[i, k] * lower[k, j]
            lower[i, j] = -running * root[i]
    for n, (i, j) in enumerate(pairs):
        total = lower[i, i] * lower[i, j]
        for k in range(i + 1, 8):
            total = total + lower[k, i] * lower[k, j]
        inv_ref[n] = total
    counts = [g_ref[8 * (72 + m) : 8 * (72 + m) + 8] for m in range(12)]
    whole = counts[0]
    for m in range(1, 12):
        whole = whole + counts[m]
    for m in range(12):
        inv_ref[36 + m] = 1.0 / jnp.maximum(counts[m], 1.0)
    inv_ref[48] = 1.0 / jnp.maximum(whole, 1.0)


def resample_body(
    foot_far,
    offs_far,
    day_far,
    smooth_far,
    scene_far,
    x_ref,
    table_far,
    foot_ref,
    offs_ref,
    day_ref,
    foot_rows,
    offs_rows,
    small_sem,
    scene,
    table_ref,
    lines,
    in_sem,
    out_sem,
):
    f32, bf16 = jnp.float32, jnp.bfloat16
    dates, bands, rows, cols = scene.shape
    parts = rows // 8
    chunks = in_sem.shape[0] - 1
    chunk = dates // chunks
    table_rows, product_rows, width = TABLE, PRODUCT, table_ref.shape[1]
    smooth_row = table_rows + product_rows
    cover_row = smooth_row + 2 * cols

    def load(k):
        part = pl.ds(k * chunk, chunk)
        return pltpu.make_async_copy(scene_far.at[part], scene.at[part], in_sem.at[k])

    smooth = pltpu.make_async_copy(
        smooth_far, table_ref.at[pl.ds(smooth_row, 2 * cols), :], in_sem.at[chunks]
    )
    load(0).start()
    small = [
        pltpu.make_async_copy(far, near, small_sem.at[k])
        for k, (far, near) in enumerate(
            (
                (day_far, day_ref),
                (foot_far, foot_ref),
                (offs_far, offs_ref),
                (foot_far, foot_rows),
                (offs_far, offs_rows),
            )
        )
    ]
    for copy in small:
        copy.start()
    for k in range(1, chunks):
        load(k).start()
    smooth.start()
    for copy in small:
        copy.wait()

    table_ref[cover_row : cover_row + TABLE, 2 * cols : 3 * cols] = jnp.zeros((TABLE, cols), bf16)
    fit_tables(day_ref, table_ref, cover_row, 2 * cols)
    strip = lane_iota((8, cols), 1) // STRIP
    span = dates * 8 // 2
    lines[...] = jnp.zeros_like(lines)
    lines[0:2, :dates] = foot_rows[...].astype(f32)
    lines[2:4, :dates] = offs_rows[...].astype(f32) * (1.0 / 16.0)
    column = lines[...].T[:EDGES]
    first, last, fy, fx = (jnp.broadcast_to(column[:, k : k + 1], (EDGES, cols)) for k in range(4))
    lane = lane_iota((EDGES, cols), 1)
    here = (lane // STRIP).astype(f32)
    for k, entry in enumerate(
        (
            fy * (1.0 - fx),
            jnp.where(lane > 0, fy * fx, 0.0),
            jnp.where((here >= first) & (here <= last), 1.0, 0.0),
        )
    ):
        table_ref[cover_row + k * EDGES : cover_row + (k + 1) * EDGES, 3 * cols : 4 * cols] = entry.astype(bf16)

    for side in range(2):

        def cover(tp, lane=side):
            tiles = []
            for u in (0, 1):
                t = lane * (span // 8) + 2 * tp + u
                inside = (strip >= foot_ref[0, t]) & (strip <= foot_ref[1, t])
                tiles.append(jnp.where(inside, 1.0, 0.0))
            row = pl.multiple_of(cover_row + 16 * tp, 16)
            table_ref[pl.ds(row, 16), lane * cols : (lane + 1) * cols] = jnp.concatenate(tiles, axis=0).astype(bf16)

        def covers(n, carry):
            for k in range(3):
                cover(3 * n + k)
            return carry

        lax.fori_loop(0, span // 48, covers, 0)
    used = cover_row + span
    smooth.wait()
    save_table = pltpu.make_async_copy(
        table_ref.at[pl.ds(0, used), :], table_far.at[pl.ds(0, used), :], out_sem.at[0]
    )
    save_table.start()

    not_last = lane_iota((8, cols), 1) < cols - 1
    bottom = lane_iota((8, cols), 0) == 7

    def splat(value):
        return jnp.full((8, cols), value, jnp.int32).astype(f32) * (1.0 / 16.0)

    def pair(tp, carry):
        fractions = []
        for u in (0, 1):
            t = 2 * tp + u
            fy, fx = splat(offs_ref[0, t]), splat(offs_ref[1, t])
            fractions.append((fy, 1.0 - fy, 1.0 - fx, jnp.where(not_last, fx, 0.0)))
        for s in range(bands):
            halves = []
            for u in (0, 1):
                fy, gy, keep, take = fractions[u]
                raw = scene[2 * tp + u, s]
                source = raw.astype(f32)
                beside = pltpu.roll(raw, cols - 1, 1).astype(f32)
                across = []
                for part in range(parts):
                    piece = source[8 * part : 8 * part + 8]
                    across.append(keep * piece + take * beside[8 * part : 8 * part + 8])
                turned = [pltpu.roll(piece, 7, 0) for piece in across]
                turned.append(0.0)
                halves.append(
                    [
                        gy * across[part] + fy * jnp.where(bottom, turned[part + 1], turned[part])
                        for part in range(parts)
                    ]
                )
            for part in range(parts):
                tile = jnp.concatenate([halves[0][part], halves[1][part]], axis=0)
                x_ref[part, s, pl.ds(pl.multiple_of(16 * tp, 16), 16), :] = tile.astype(bf16)
        return carry

    for k in range(chunks):
        load(k).wait()
        lax.fori_loop(k * chunk // 2, (k + 1) * chunk // 2, pair, 0)
    save_table.wait()


def fit_body(
    words,
    place_ref,
    bits_ref,
    below_ref,
    x_ref,
    table_far,
    send_ref,
    table_ref,
    below_wide,
    edge_ref,
    b8,
    bfull,
    wc_ref,
    w_ref,
    g_ref,
    inv_ref,
    wide_ref,
    y_ref,
    in_sem,
):
    f32, bf16 = jnp.float32, jnp.bfloat16
    dates, bands, cols = below_ref.shape
    cells_here = b8.shape[1]
    steps, _, _, wide = bfull.shape
    group = wide // cols
    parts = steps * group
    rows = 8 * parts
    half = cells_here // parts
    depth, width = 8 * dates, table_ref.shape[1]
    smooth_row = TABLE + PRODUCT
    cover_row = smooth_row + 2 * cols
    span = depth // words
    arrivals = [
        pltpu.make_async_copy(table_far.at[part, :], table_ref.at[part, :], in_sem.at[k])
        for k, part in enumerate((pl.ds(cover_row, span), pl.ds(0, cover_row)))
    ]
    for copy in arrivals:
        copy.start()

    own_words(words, place_ref[0] * cells_here, bits_ref, b8)
    y_ref[y_ref.shape[0] - 1] = jnp.zeros(y_ref.shape[1:], bf16)
    top = lane_iota((8, cols), 0) < 8 // half
    for w in range(words):
        for part in range(parts):
            q, g = divmod(part, group)
            bfull[q, w, :, g * cols : (g + 1) * cols] = jnp.where(
                top, b8[w, part * half : part * half + 1, :], b8[w, part * half + 1 : part * half + 2, :]
            )

    def spread_rows(n, carry):
        for k in range(6):
            t = 6 * n + k
            below_wide[pl.ds(pl.multiple_of(8 * t, 8), bands), :] = below_ref[t].astype(f32)
        return carry

    lax.fori_loop(0, dates // 6, spread_rows, 0)
    arrivals[0].wait()
    per_word = dates // words
    when = lane_iota((EDGES, cols), 0)
    word = b8[0, cells_here - 1 : cells_here, :]
    for w in range(1, words):
        word = jnp.where(when >= w * per_word, b8[w, cells_here - 1 : cells_here, :], word)
    flag = (lax.shift_right_logical(jnp.broadcast_to(word, (EDGES, cols)), when % per_word) & 1).astype(f32)
    near, far, cover = (
        table_ref[cover_row + k * EDGES : cover_row + (k + 1) * EDGES, 3 * cols : 4 * cols].astype(f32)
        for k in range(3)
    )
    flag = flag * cover
    near, far = near * flag, far
    for s in range(bands):
        row = below_wide[pl.ds(s, EDGES, stride=8), :]
        edge = near * row + flag * pltpu.roll(far * row, cols - 1, 1)
        edge_ref[s] = jnp.where(when < dates, edge, 0.0).astype(bf16)
    for lane in range(words):

        def mask_pair(tp, lane=lane):
            cover = table_ref[pl.ds(pl.multiple_of(cover_row + 16 * tp, 16), 16), lane * cols : (lane + 1) * cols]
            first = lane * (span // 8) + 2 * tp
            w = first // per_word
            coarse = b8[w]
            fine = [bfull[q, w] for q in range(steps)]
            small, large = [], [[] for _ in range(steps)]
            for u in (0, 1):
                bit = jnp.left_shift(1, first + u - w * per_word)
                small.append(jnp.where((coarse & bit) != 0, 1.0, 0.0))
                for q in range(steps):
                    large[q].append(jnp.where((fine[q] & bit) != 0, 1.0, 0.0))
            row = pl.ds(pl.multiple_of(lane * span + 16 * tp, 16), 16)
            wc_ref[row, :] = jnp.concatenate(small, axis=0).astype(bf16) * cover
            for q in range(steps):
                both = jnp.concatenate(large[q], axis=0).astype(bf16)
                w_ref[q, row, :] = both * jnp.concatenate([cover] * group, axis=1)

        def mask_pairs(n, carry):
            for k in range(3):
                mask_pair(3 * n + k)
            return carry

        lax.fori_loop(0, span // 48, mask_pairs, 0)
    arrivals[1].wait()
    g_ref[...] = jnp.dot(table_ref[TABLE:smooth_row, :depth], wc_ref[...], preferred_element_type=f32)
    solve_cells(g_ref, inv_ref)

    def widen(block, carry):
        for k in range(7):
            n = 7 * block + k
            for part in range(parts):
                q, g = divmod(part, group)
                wide_ref[q, n, :, g * cols : (g + 1) * cols] = jnp.where(
                    top,
                    inv_ref[n, part * half : part * half + 1, :],
                    inv_ref[n, part * half + 1 : part * half + 2, :],
                )
        return carry

    lax.fori_loop(0, inv_ref.shape[0] // 7, widen, 0)


    coef_groups = cdiv(8 * bands, 16)
    order = {}
    for i in range(8):
        for j in range(i + 1):
            order[i, j] = order[j, i] = len(set(order.values()))

    def sums_of(q, s):
        weighted = jnp.concatenate([x_ref[q * group + g, s] for g in range(group)], axis=1) * w_ref[q]
        sums = jnp.dot(table_ref[:TABLE, :depth], weighted, preferred_element_type=f32)
        if q == steps - 1:
            edge = jnp.concatenate([jnp.zeros((EDGES, (group - 1) * cols), bf16), edge_ref[s]], axis=1)
            near_edge = table_ref[cover_row : cover_row + TABLE, 2 * cols : 2 * cols + EDGES]
            sums = sums + jnp.dot(near_edge, edge, preferred_element_type=f32)
        return sums

    def put(q, base, e, u, value):
        tall = jnp.concatenate([value[:, g * cols : (g + 1) * cols] for g in range(group)], axis=0)
        row = u % 8 * rows + q * group * 8
        y_ref[base + u // 8, row : row + group * 8, e * cols : (e + 1) * cols] = tall.astype(bf16)

    def use(q, s, sums):
        month = [sums[8 * (14 + m) : 8 * (14 + m) + 8] for m in range(12)]
        whole = month[0]
        for m in range(1, 12):
            whole = whole + month[m]
        rhs = [whole] + [sums[8 * k : 8 * k + 8] + sums[8 * (k + 7) : 8 * (k + 7) + 8] for k in range(7)]
        for m in range(12):
            put(q, coef_groups, m % 2, (m // 2) * bands + s, month[m] * wide_ref[q, 36 + m])
        put(q, coef_groups, s % 2, 6 * bands + s // 2, whole * wide_ref[q, 48])
        for i in range(8):
            value = wide_ref[q, order[i, 0]] * rhs[0]
            for j in range(1, 8):
                value = value + wide_ref[q, order[i, j]] * rhs[j]
            put(q, 0, i % 2, (i // 2) * bands + s, value)

    places = [(q, s) for q in range(steps) for s in range(bands)]
    waiting = sums_of(*places[0])
    for n, (q, s) in enumerate(places):
        ready = waiting
        if n + 1 < len(places):
            waiting = sums_of(*places[n + 1])
        use(q, s, ready)

    for at in range(y_ref.shape[0]):
        side = 0 if at < coef_groups else 2 * cols
        turned = lax.dot_general(
            table_ref[smooth_row:cover_row, side : side + 2 * cols],
            y_ref[at],
            (((1,), (1,)), ((), ())),
            preferred_element_type=f32,
        ).reshape(cols // STRIP, 2 * STRIP, 2 * cols)
        tile = jnp.concatenate([turned[:, :, :cols], turned[:, :, cols:]], axis=1)
        send_ref[:, 16 * at : 16 * at + 16, :] = tile.astype(bf16)


def finish_body(bands, recv_ref, coef_ref, month_ref, year_ref, field_ref, out_sem):
    strips, slots, lanes = recv_ref.shape
    groups = slots // 16
    coef_groups = cdiv(8 * bands, 16)
    quarter = lanes // 4
    lane = lane_iota((16, lanes), 1)
    low_half = lane < 2 * quarter
    even = lane // quarter % 2 == 0

    def save(k):
        first, count, target = (
            (0, 8 * bands, coef_ref),
            (8 * bands, 8 * bands, month_ref.at[pl.ds(0, 8 * bands)]),
            (16 * bands, 4 * bands, month_ref.at[pl.ds(8 * bands, 4 * bands)]),
            (20 * bands, bands, year_ref),
        )[k]
        return pltpu.make_async_copy(field_ref.at[pl.ds(first, count)], target, out_sem.at[k])

    def one_group(is_coef, at, carry):
        part = pl.ds(pl.multiple_of(16 * at, 16), 16)
        tiles = []
        for lt in range(strips // 4):
            x = [recv_ref[4 * lt + b, part, :] for b in range(4)]
            for b in (0, 1):
                first, second = x[b], x[b + 2]
                x[b] = jnp.where(low_half, first, pltpu.roll(second, 2 * quarter, 1))
                x[b + 2] = jnp.where(low_half, pltpu.roll(first, 2 * quarter, 1), second)
            for b in (0, 2):
                first, second = x[b], x[b + 1]
                x[b] = jnp.where(even, first, pltpu.roll(second, quarter, 1))
                x[b + 1] = jnp.where(even, pltpu.roll(first, 3 * quarter, 1), second)
            tiles.append(x)
        for p in range(4):
            field = jnp.concatenate([tile[p].astype(jnp.float32) for tile in tiles], axis=1)
            if not is_coef:
                full = field.shape[1]
                where = lane_iota(field.shape, 1)
                before = jnp.where(where == 0, 0.0, pltpu.roll(field, 1, 1))
                after = jnp.where(where == full - 1, 0.0, pltpu.roll(field, full - 1, 1))
                field = 0.25 * before + 0.5 * field + 0.25 * after
            for h in (0, 1):
                u = 8 * at + 4 * h + p
                late = u - 8 * coef_groups
                for e in (0, 1):
                    coef = (2 * (u // bands) + e) * bands + lax.rem(u, bands)
                    month = (2 * (late // bands) + e) * bands + lax.rem(late, bands)
                    mean = 2 * (late - 6 * bands) + e
                    v = coef if is_coef else jnp.where(late < 6 * bands, 8 * bands + month, 20 * bands + mean)
                    field_ref[v] = field[8 * h + 4 * e : 8 * h + 4 * e + 4]
        return carry

    lax.fori_loop(0, coef_groups, functools.partial(one_group, True), 0)
    save(0).start()
    early = coef_groups + 4 * bands // 8
    lax.fori_loop(coef_groups, early, functools.partial(one_group, False), 0)
    save(1).start()
    lax.fori_loop(early, groups, functools.partial(one_group, False), 0)
    save(2).start()
    save(3).start()
    for k in range(4):
        save(k).wait()


def turn_tables(strips, strip_width):
    cols = strips * strip_width
    row, col = np.arange(2 * cols)[:, None], np.arange(2 * cols)[None, :]
    column = strip_width * (row // (2 * strip_width)) + row % strip_width
    same = row // strip_width % 2 == col // cols
    apart = np.abs(column - col % cols)
    plain = np.where(same & (apart == 0), 1.0, 0.0)
    smooth = np.where(same, np.where(apart == 0, 0.5, np.where(apart == 1, 0.25, 0.0)), 0.0)
    return jnp.asarray(np.concatenate([plain, smooth], axis=1), jnp.bfloat16)


def whole_dates(scenes, clear_bits, footprint, offsets, acq_day):
    dates, bands, rows, cols = scenes.shape
    words, _, cells = clear_bits.shape
    strips = lax.axis_size("band")
    cells_here = cells // strips
    group, lanes, chunks = 2, 128, 3
    steps = rows // 8 // group
    depth, wide = 8 * dates, group * cols
    f32, bf16 = jnp.float32, jnp.bfloat16
    blocks = words * cells // lanes
    flags = jnp.broadcast_to(clear_bits.reshape(1, blocks, 1, lanes), (strips, blocks, 1, lanes))
    flags = lax.all_to_all(flags, "band", split_axis=0, concat_axis=0, tiled=True)
    below = shifted(scenes[:, :, 0, :], "band", -1)
    smem = pl.BlockSpec(memory_space=pltpu.SMEM)
    vmem = pl.BlockSpec(memory_space=pltpu.VMEM)
    anywhere = pl.BlockSpec(memory_space=pl.ANY)
    far = pl.BlockSpec(memory_space=pltpu.HBM)
    groups = cdiv(8 * bands, 16) + cdiv(13 * bands, 16)
    place = lax.axis_index("band").reshape(1).astype(jnp.int32)
    parts, table_width = rows // 8, 4 * cols
    x_shape = (parts, bands, depth, cols)
    table_shape = (TABLE + PRODUCT + 4 * cols + 16, table_width)
    def pinned(x):
        return pltpu.with_memory_space_constraint(x, pltpu.HBM)

    resampled, table = pl.pallas_call(
        resample_body,
        in_specs=[far] * 5,
        out_specs=[vmem, far],
        out_shape=[
            jax.ShapeDtypeStruct(x_shape, bf16),
            pltpu.HBM(table_shape, bf16),
        ],
        scratch_shapes=[
            pltpu.SMEM((2, dates), jnp.int32),
            pltpu.SMEM((2, dates), jnp.int32),
            pltpu.VMEM((1, dates), jnp.int32),
            pltpu.VMEM((2, dates), jnp.int32),
            pltpu.VMEM((2, dates), jnp.int32),
            pltpu.SemaphoreType.DMA((5,)),
            pltpu.VMEM(scenes.shape, bf16),
            pltpu.VMEM(table_shape, bf16),
            pltpu.VMEM((8, 128), f32),
            pltpu.SemaphoreType.DMA((chunks + 1,)),
            pltpu.SemaphoreType.DMA((1,)),
        ],
        compiler_params=pltpu.CompilerParams(vmem_limit_bytes=RESAMPLE_VMEM),
        cost_estimate=pl.CostEstimate(flops=20_000_000, bytes_accessed=9_000_000, transcendentals=0),
        name="resample",
    )(*(pinned(x) for x in (footprint.T, offsets.T, acq_day.reshape(1, dates), turn_tables(strips, STRIP), scenes)))
    send = pl.pallas_call(
        functools.partial(fit_body, words),
        in_specs=[smem, vmem, vmem, vmem, far],
        out_specs=vmem,
        out_shape=jax.ShapeDtypeStruct((strips, 16 * groups, 4 * rows), bf16),
        scratch_shapes=[
            pltpu.VMEM(table_shape, bf16),
            pltpu.VMEM((8 * EDGES, cols), f32),
            pltpu.VMEM((bands, EDGES, cols), bf16),
            pltpu.VMEM((words, cells_here, cols), jnp.int32),
            pltpu.VMEM((steps, words, 8, wide), jnp.int32),
            pltpu.VMEM((depth, cols), bf16),
            pltpu.VMEM((steps, depth, wide), bf16),
            pltpu.VMEM((PRODUCT, cols), f32),
            pltpu.VMEM((49, cells_here, cols), f32),
            pltpu.VMEM((steps, 49, 8, wide), f32),
            pltpu.VMEM((groups, 8 * rows, 2 * cols), bf16),
            pltpu.SemaphoreType.DMA((2,)),
        ],
        compiler_params=pltpu.CompilerParams(vmem_limit_bytes=FIT_VMEM),
        cost_estimate=pl.CostEstimate(flops=20_000_000, bytes_accessed=6_000_000, transcendentals=0),
        name="fit",
    )(place, flags.reshape(strips * blocks, lanes), below, resampled, pinned(table))
    received = lax.all_to_all(send, "band", split_axis=0, concat_axis=0, tiled=True)
    row_count = rows * strips
    shapes = [(n * bands, STRIP, row_count) for n in (8, 12, 1)]
    coefficients, monthly, annual = pl.pallas_call(
        functools.partial(finish_body, bands),
        in_specs=[vmem],
        out_specs=[anywhere] * 3,
        out_shape=[jax.ShapeDtypeStruct(shape, f32) for shape in shapes],
        scratch_shapes=[
            pltpu.VMEM((16 * groups, STRIP, row_count), f32),
            pltpu.SemaphoreType.DMA((4,)),
        ],
        compiler_params=pltpu.CompilerParams(vmem_limit_bytes=8 << 20),
        name="finish",
    )(received)
    return (
        coefficients.reshape(8, bands, STRIP, row_count),
        monthly.reshape(12, bands, STRIP, row_count),
        annual,
    )


def shards(scenes, clear_bits, footprint, offsets, acq_day):
    dates, bands, rows, cols = scenes.shape
    strips = lax.axis_size("band")
    words, _, cells = clear_bits.shape
    whole = (
        lax.axis_size("tile") == 1
        and cols == 128
        and rows == 32
        and cols == STRIP * strips
        and cells == 8 * strips
        and words == 2
        and dates == 30 * words
        and dates % 12 == 0
        and dates <= 60
        and bands % 6 == 0
        and bands <= 6
    )
    plan = whole_dates if whole else split_dates
    return plan(scenes, clear_bits, footprint, offsets, acq_day)


def solution(mesh):
    placed = (
        P(("region", "tile"), "sub", "band", None),
        P(("region", "tile"), "band", None),
        P(("region", "tile"), None),
        P(("region", "tile"), None),
        P(("region", "tile")),
    )
    return jax.shard_map(
        shards,
        mesh=mesh,
        in_specs=placed,
        out_specs=(
            P("region", "sub", "band", "tile"),
            P(("region", "tile"), "sub", "band", None),
            P(("region", "sub"), "band", "tile"),
        ),
        check_vma=False,
    )
```
